256 devices in a mesh: nx: 8 (over x, core), ny: 16 (over y_lo, z), img: 2 (over y_hi).
Axes of the slice: x: 4, y: 4 (y_hi: 2, y_lo: 2; y = y_hi * 2 + y_lo), z: 8, core: 2. Of those that a mesh axis runs over, the one named last changes fastest.
Arguments:
- features: bfloat16 [256, 65536], P(('nx', 'ny', 'img')), may hold values from 0 to 2
- link_weight: bfloat16 [3, 128, 128, 128, 128], P(None, ('nx', 'ny')), may hold values from -0.1875 to 0.1875
- link_row: int32 [3, 128, 128], P(None, ('nx', 'ny')), may hold values from 0 to 3
- link_col: int32 [3, 128, 128], P(None, None, ('nx', 'ny')), may hold values from 0 to 3
- link_live: int32 [3, 128, 128], P(None, ('nx', 'ny')), may hold values from 0 to 1, as said below
- bias: float32 [3, 65536], P(None, ('nx', 'ny')), may hold values from -3 to 3
Outputs:
- activations: bfloat16 [256, 65536], P(('nx', 'ny', 'img'))
The draws below stay inside these ranges and needn't reach their ends.
Inputs may be any that keep to these rules, and one draw needn't show every extreme that they name: `link_live`: in every layer at most 96 of the links of one source device are live, and exactly 96 for some source device.
All inputs are finite; a program needn't handle non-finite values.
Results may differ from the reference program's by a relative error of at most 0.0072.
Values may be sent and summed in bfloat16 or wider, within the bound.
A program may use at most 64 MiB of HBM per device.

```python
import jax
import jax.numpy as jnp
from jax import lax

BLK = 128
NB_DEV = 4
LAYERS = 3
LINKS = 128
IMAGES = 256
NEURONS = 65536
LIVE_MAX = 96


def draw_link_live(key, part):
    key_count = jax.random.fold_in(key, 11)
    key_busy = jax.random.fold_in(key, 12)
    key_perm = jax.random.fold_in(key, 13)
    live_counts = jax.random.randint(key_count, (LAYERS, LINKS), LINKS // 4, LIVE_MAX + 1)
    busiest = jax.random.randint(key_busy, (LAYERS,), 0, LINKS)
    positions = jnp.arange(LINKS, dtype=jnp.int32)
    live_counts = jnp.where(positions[None, :] == busiest[:, None], LIVE_MAX, live_counts)
    perm_keys = jax.random.split(key_perm, LAYERS * LINKS)
    ranking = jax.vmap(lambda subkey: jax.random.permutation(subkey, LINKS))(perm_keys)
    ranking = ranking.reshape(LAYERS, LINKS, LINKS)
    return (ranking < live_counts[:, :, None]).astype(jnp.int32)


def touch_ends(array, key, least, top_value):
    longest = array.shape.index(max(array.shape))
    spots = []
    for shift in (0, 1):
        where = [jax.random.randint(jax.random.fold_in(key, axis), (), 0, length) for axis, length in enumerate(array.shape)]
        where[longest] = (where[longest] + shift) % array.shape[longest]
        spots.append(tuple(where))
    return array.at[spots[0]].set(least).at[spots[1]].set(top_value)


def block_levels(key, shape, pieces, least, high):
    def one(axis_at, shards_of):
        heights = jax.random.uniform(jax.random.fold_in(jax.random.fold_in(key, 6), axis_at), (shards_of,), jnp.float32, least / len(pieces), high / len(pieces))
        return jnp.repeat(jnp.exp(heights), shape[axis_at] // shards_of).reshape((-1,) + (1,) * (len(shape) - axis_at - 1))

    level = one(*pieces[0])
    for cut in pieces[1:]:
        level = level * one(*cut)
    return level


def noise(key, extent, scale, bound, cuts=(), kind=jnp.bfloat16):
    result = jax.random.normal(key, extent, jnp.float32) * scale
    if len(cuts) > 0:
        result = block_levels(key, extent, cuts, -0.22, 0.18) * result
    return jnp.clip(result, min=-bound, max=bound).astype(kind)


def setup_inputs(seed: int = 0) -> dict:
    streams_of = jax.random.split(jax.random.key(seed), 7)
    features = jnp.clip(2.0 * jax.random.uniform(streams_of[0], (IMAGES, NEURONS), jnp.float32) ** block_levels(streams_of[0], (IMAGES, NEURONS), ((0, 256),), -0.2, 0.2), 0.0, 2.0).astype(jnp.bfloat16)
    link_weight = noise(streams_of[1], (LAYERS, LINKS, LINKS, BLK, BLK), (LINKS * BLK // 16) ** -0.5, 0.1875, ((1, 128),))
    link_row = touch_ends(jax.random.randint(streams_of[2], (LAYERS, LINKS, LINKS), 0, NB_DEV), jax.random.fold_in(streams_of[2], 1), 0, NB_DEV - 1).astype(jnp.int32)
    link_col = touch_ends(jax.random.randint(streams_of[3], (LAYERS, LINKS, LINKS), 0, NB_DEV), jax.random.fold_in(streams_of[3], 1), 0, NB_DEV - 1).astype(jnp.int32)
    link_live = draw_link_live(jax.random.fold_in(streams_of[6], 71), 0)
    bias = noise(streams_of[5], (LAYERS, NEURONS), 0.5, 3.0, ((1, 128),), jnp.float32)
    return dict(features=features, link_weight=link_weight, link_row=link_row, link_col=link_col, link_live=link_live, bias=bias)


def reference(features, link_weight, link_row, link_col, link_live, bias):
    images = features.shape[0]
    nblocks = NB_DEV * LINKS
    hidden = features.reshape(images, LINKS, NB_DEV, BLK)
    for layer_idx in range(LAYERS):
        def one_source(running, inputs_now):
            source, weights, row_ids, live_mask, col_ids = inputs_now
            blocks = lax.dynamic_index_in_dim(hidden, source, 1, keepdims=False)
            masked = weights * live_mask.astype(jnp.bfloat16)[:, None, None]
            gathered = jnp.take(blocks, row_ids, axis=1)
            link_terms = jnp.einsum("ier,ers->ies", gathered.astype(jnp.float32), masked.astype(jnp.float32)).astype(jnp.bfloat16)
            targets = (jnp.arange(LINKS, dtype=jnp.int32) * NB_DEV + col_ids).astype(jnp.int32)
            running = running.at[:, targets].add(link_terms.astype(jnp.float32))
            return running, None

        sources = jnp.arange(LINKS, dtype=jnp.int32)
        start = jnp.zeros((images, nblocks, BLK), jnp.float32)
        running, unused = lax.scan(one_source, start, (sources, link_weight[layer_idx], link_row[layer_idx], link_live[layer_idx], link_col[layer_idx]))
        pre_sum = running.reshape(images, nblocks * BLK) + bias[layer_idx][None, :]
        hidden = jnp.maximum(pre_sum, 0.0).astype(jnp.bfloat16).reshape(images, LINKS, NB_DEV, BLK)
    return hidden.reshape(images, nblocks * BLK)
```

```python
import jax
import jax.numpy as jnp
from jax import lax
from jax.experimental import pallas as pl
from jax.experimental.pallas import tpu as pltpu
from jax.sharding import PartitionSpec as P

MESH = pl.DeviceIdType.MESH
NXC, NZ = 4, 8


def layers_kernel(w_hbm, h0, meta, bias, out, wbuf, act, work, ybuf, r1, r2, zr, metav, colv, metas, cols,
                  wl_sem, ws_sem, wr_sem, ms_sem, mr_sem, cs_sem, cr_sem, loc_sem,
                  ag_s, ag_r, xs_sem, x1_r, x2_r, zs_sem, z_r):
    f32, bf16 = jnp.float32, jnp.bfloat16
    nx, ny, im = lax.axis_index("nx"), lax.axis_index("ny"), lax.axis_index("img")
    x, c = nx // 2, nx % 2
    yl, z = ny // NZ, ny % NZ
    me = yl * 2 + c
    plane = x * NZ + z
    layers = act.shape[0] - 1

    def dev(xx, cc, yy, zz, ii):
        return (xx * 2 + cc, yy * NZ + zz, ii)

    partner = dev(x, 1 - c, yl, z, im)
    near = dev(x, c, 1 - yl, z, im)
    im_up = (im + yl) % 2
    im_dn = (im + 1 - yl) % 2
    xp = dev((x + 1) % NXC, c, yl, z, im)
    xm = dev((x + NXC - 1) % NXC, c, yl, z, im)
    zp = dev(x, c, yl, (z + 1) % NZ, im)
    zm = dev(x, c, yl, (z + NZ - 1) % NZ, im)

    def in_plane(j):
        return dev((x + j // NZ) % NXC, c, yl, (z + j) % NZ, im)

    barrier = pltpu.get_barrier_semaphore()

    def greet(d):
        pl.semaphore_signal(barrier, inc=1, device_id=d, device_id_type=MESH)

    greet(partner)
    for cc in (0, 1):
        greet(dev(x, cc, 1 - yl, z, im_up))
        greet(dev(x, cc, 1 - yl, z, im_dn))

    def greet_plane(j, carry):
        greet(in_plane(j))
        return carry

    lax.fori_loop(1, NXC * NZ, greet_plane, 0)
    pl.semaphore_wait(barrier, 5 + NXC * NZ - 1)

    def remote(src, dst, ss, rs, d):
        return pltpu.make_async_remote_copy(src_ref=src, dst_ref=dst, send_sem=ss, recv_sem=rs,
                                            device_id=d, device_id_type=MESH)

    def w_remote(l, xx, cc, yy, ii, slot):
        first = (xx * 2 + cc) * 2 * NZ + yy * NZ
        return remote(w_hbm.at[l, pl.ds(first, NZ)], wbuf.at[l, me, pl.ds(xx * NZ, NZ)],
                      ws_sem.at[l, slot], wr_sem.at[l, me, xx], dev(x, cc, yy, z, ii))

    def w_copies(l):
        res = []
        for xx in range(NXC):
            res.append(w_remote(l, xx, 1 - c, yl, im, xx))
        for i in range(2):
            for cc in (0, 1):
                res.append(w_remote(l, i, cc, 1 - yl, im_up, 4 + 2 * i + cc))
                res.append(w_remote(l, 2 + i, cc, 1 - yl, im_dn, 8 + 2 * i + cc))
        return res

    def w_local(l, xx):
        first = (xx * 2 + c) * 2 * NZ + yl * NZ
        return pltpu.make_async_copy(w_hbm.at[l, pl.ds(first, NZ)], wbuf.at[l, me, pl.ds(xx * NZ, NZ)],
                                     wl_sem.at[l, xx])

    def start_weights(l):
        for cp in w_copies(l):
            cp.start()
        for xx in range(NXC):
            w_local(l, xx).start()

    def wait_weights(l):
        for xx in range(NXC):
            w_local(l, xx).wait()
        for k in range(1, 4):
            src = (me + k) % 4
            for xx in range(NXC):
                remote(w_hbm.at[l, pl.ds(0, NZ)], wbuf.at[l, src, pl.ds(xx * NZ, NZ)],
                       ws_sem.at[l, 0], wr_sem.at[l, src, xx], partner).wait_recv()

    def ag(l, src, slot, d):
        return remote(act.at[l, src], act.at[l, src], ag_s.at[l, slot], ag_r.at[l, slot], d)

    def gather_start(l):
        ag(l, me, 0, near).start()
        ag(l, me, 1, partner).start()

    nb = (1 - yl) * 2 + c

    def gather_finish(l):
        ag(l, nb, 0, near).wait_recv()
        ag(l, nb, 2, partner).start()
        ag(l, yl * 2 + 1 - c, 1, partner).wait_recv()
        ag(l, (1 - yl) * 2 + 1 - c, 2, partner).wait_recv()
        ag(l, me, 0, near).wait_send()
        ag(l, me, 1, partner).wait_send()
        ag(l, nb, 2, partner).wait_send()

    metav[me] = meta[pl.ds(0, 8), :]
    colv[plane] = meta[pl.ds(8, 8), :]
    act[0, me] = h0[...]

    def meta_cp(k, d):
        return remote(meta.at[pl.ds(0, 8)], metav.at[me], ms_sem.at[k], mr_sem.at[k], d)

    def col_cp(j):
        return remote(meta.at[pl.ds(8, 8)], colv.at[plane], cs_sem.at[j], cr_sem.at[j], in_plane(j))

    meta_cp(0, partner).start()
    meta_cp(1, near).start()
    meta_cp(2, dev(x, 1 - c, 1 - yl, z, im)).start()
    gather_start(0)

    def send_col(j, carry):
        col_cp(j).start()
        return carry

    lax.fori_loop(1, NXC * NZ, send_col, 0)
    start_weights(0)
    gather_finish(0)
    for k, d, src in ((0, partner, yl * 2 + 1 - c), (1, near, nb), (2, dev(x, 1 - c, 1 - yl, z, im), (1 - yl) * 2 + 1 - c)):
        remote(meta.at[pl.ds(0, 8)], metav.at[src], ms_sem.at[k], mr_sem.at[k], d).wait_recv()
        meta_cp(k, d).wait_send()

    def wait_col(j, carry):
        frm = ((x + NXC - j // NZ) % NXC) * NZ + (z + NZ - j % NZ) % NZ
        remote(meta.at[pl.ds(8, 8)], colv.at[frm], cs_sem.at[j], cr_sem.at[j], in_plane(j)).wait_recv()
        col_cp(j).wait_send()
        return carry

    lax.fori_loop(1, NXC * NZ, wait_col, 0)
    cp = pltpu.make_async_copy(metav, metas, loc_sem.at[0])
    cp2 = pltpu.make_async_copy(colv, cols, loc_sem.at[1])
    cp.start()
    cp2.start()
    cp.wait()
    cp2.wait()

    za = [(z + 4 - j) % NZ for j in range(4)]
    zb = [(z + NZ - 3 + j) % NZ for j in range(4)]
    x1, x2, x3 = (x + 1) % NXC, (x + 2) % NXC, (x + 3) % NXC

    def layer(l, carry):
        @pl.when(l > 0)
        def _():
            gather_finish(l)

        @pl.when(l < layers - 1)
        def _():
            start_weights(l + 1)

        wait_weights(l)
        for s in range(4):
            work[s] = act[l, s]

        def one(e, carry):
            dest = ((e // NZ) * 2 + c) * 2 * NZ + yl * NZ + e % NZ
            lhs, rhs = [], []
            for s in range(4):
                src = (x * 2 + s % 2) * 2 * NZ + (s // 2) * NZ + z
                row, live, col = metas[s, l, dest], metas[s, 3 + l, dest], cols[e, l, src]
                lhs.append(work[s, row])
                block = wbuf[l, s, e]
                key = jnp.where(live == 1, col, 4)
                rhs.append(jnp.concatenate(
                    [jnp.where(key == k, block, jnp.zeros_like(block)) for k in range(4)], axis=1))
            res = jnp.dot(jnp.concatenate(lhs, axis=1), jnp.concatenate(rhs, axis=0), preferred_element_type=f32)
            for k in range(4):
                ybuf[e // NZ, e % NZ, k] = res[:, k * 128:(k + 1) * 128].astype(bf16)
            return carry

        lax.fori_loop(0, NXC * NZ, one, 0)

        def s1(side, j):
            zz = za[j] if side == 0 else zb[j]
            return remote(ybuf.at[x2, zz], r1.at[l, side, j], xs_sem.at[l, side, j], x1_r.at[l, side, j],
                          xp if side == 0 else xm)

        def s2(side, p):
            zz = za[p] if p < 4 else zb[p - 4]
            return remote(ybuf.at[x1 if side == 0 else x3, zz], r2.at[l, side, p], xs_sem.at[l, side, 4 + p],
                          x2_r.at[l, side, p], xp if side == 0 else xm)

        for j in range(4):
            s1(0, j).start()
            s1(1, j).start()
        for j in range(4):
            s2(0, 4 + j).start()
            s2(1, j).start()
            for side, p in ((0, j), (1, 4 + j)):
                s1(side, j).wait_recv()
                xx, zz = (x1, za[j]) if side == 0 else (x3, zb[j])
                ybuf[xx, zz] = (ybuf[xx, zz].astype(f32) + r1[l, side, j].astype(f32)).astype(bf16)
                s2(side, p).start()

        def zcp(side, o):
            d, slot = (zp, 4 - o) if side == 0 else (zm, 4 + 3 + o)
            zz = (z + o + NZ) % NZ
            return remote(ybuf.at[x, zz], zr.at[l, slot], zs_sem.at[l, slot], z_r.at[l, slot], d)

        def total(p, zz):
            s2(0, p).wait_recv()
            s2(1, p).wait_recv()
            return (ybuf[x, zz].astype(f32) + r2[l, 0, p].astype(f32)) + r2[l, 1, p].astype(f32)

        for j in range(4):
            acc = total(j, za[j])
            if j > 0:
                zcp(0, 5 - j).wait_recv()
                acc = acc + zr[l, j - 1].astype(f32)
            ybuf[x, za[j]] = acc.astype(bf16)
            zcp(0, 4 - j).start()
            acc = total(4 + j, zb[j])
            if j > 0:
                zcp(1, -4 + j).wait_recv()
                acc = acc + zr[l, 4 + j - 1].astype(f32)
            if j < 3:
                ybuf[x, zb[j]] = acc.astype(bf16)
                zcp(1, -3 + j).start()
        zcp(0, 1).wait_recv()
        pre = acc + zr[l, 3].astype(f32) + bias[l]
        act[l + 1, me] = jnp.maximum(pre, 0.0).astype(bf16)

        @pl.when(l < layers - 1)
        def _():
            gather_start(l + 1)

        for side in (0, 1):
            for j in range(4):
                s1(side, j).wait_send()
            for p in range(8):
                s2(side, p).wait_send()
        for j in range(4):
            zcp(0, 4 - j).wait_send()
            if j < 3:
                zcp(1, -3 + j).wait_send()
        for cp in w_copies(l):
            cp.wait_send()
        return carry

    lax.fori_loop(0, layers, layer, 0)
    out[...] = act[layers, me]


def run_layers(w, h0, meta, bias):
    layers, half = w.shape[0], h0.shape[1]
    bf16, DMA = jnp.bfloat16, pltpu.SemaphoreType.DMA
    piece = (4, half, 128)
    vm = pl.BlockSpec(memory_space=pltpu.VMEM)
    return pl.pallas_call(
        layers_kernel,
        out_shape=jax.ShapeDtypeStruct(piece, bf16),
        in_specs=[pl.BlockSpec(memory_space=pl.ANY), vm, vm, vm],
        out_specs=vm,
        scratch_shapes=[
            pltpu.VMEM((layers, 4, NXC * NZ, 128, 128), bf16),
            pltpu.VMEM((layers + 1, 4) + piece, bf16),
            pltpu.VMEM((4,) + piece, bf16),
            pltpu.VMEM((NXC, NZ) + piece, bf16),
            pltpu.VMEM((layers, 2, 4) + piece, bf16),
            pltpu.VMEM((layers, 2, 8) + piece, bf16),
            pltpu.VMEM((layers, 7) + piece, bf16),
            pltpu.VMEM((4, 8, 128), jnp.int32),
            pltpu.VMEM((NXC * NZ, 8, 128), jnp.int32),
            pltpu.SMEM((4, 8, 128), jnp.int32),
            pltpu.SMEM((NXC * NZ, 8, 128), jnp.int32),
            DMA((layers, 4)), DMA((layers, 12)), DMA((layers, 4, 4)),
            DMA((3,)), DMA((3,)), DMA((NXC * NZ,)), DMA((NXC * NZ,)), DMA((2,)),
            DMA((layers, 3)), DMA((layers, 3)),
            DMA((layers, 2, 12)), DMA((layers, 2, 4)), DMA((layers, 2, 8)),
            DMA((layers, 7)), DMA((layers, 7)),
        ],
        compiler_params=pltpu.CompilerParams(
            collective_id=0, has_side_effects=True, vmem_limit_bytes=56 * 1024 * 1024),
    )(w, h0, meta, bias)


def local(features, link_weight, link_row, link_col, link_live, bias):
    hidden = lax.all_to_all(features, ("nx", "ny"), split_axis=1, concat_axis=0, tiled=True)
    rows = hidden.shape[0]
    h0 = hidden.reshape(rows, 4, 128).transpose(1, 0, 2)
    two = jnp.zeros((2, 128), jnp.int32)
    five = jnp.zeros((5, 128), jnp.int32)
    meta = jnp.concatenate([link_row[:, 0], link_live[:, 0], two, link_col[:, :, 0], five], axis=0)
    res = run_layers(link_weight[:, 0], h0, meta, bias.reshape(bias.shape[0], 4, 1, 128))
    hidden = res.transpose(1, 0, 2).reshape(rows, 512)
    return lax.all_to_all(hidden, ("nx", "ny"), split_axis=0, concat_axis=1, tiled=True)


def solution(mesh):
    placed = (
        P(("nx", "ny", "img"), None),
        P(None, ("nx", "ny"), None, None, None),
        P(None, ("nx", "ny"), None),
        P(None, None, ("nx", "ny")),
        P(None, ("nx", "ny"), None),
        P(None, ("nx", "ny")),
    )
    return jax.shard_map(
        local, mesh=mesh, in_specs=placed, out_specs=P(("nx", "ny", "img"), None), check_vma=False
    )
```

```python
import jax
import jax.numpy as jnp
from jax import lax
from jax.experimental import pallas as pl
from jax.experimental.pallas import tpu as pltpu
from jax.sharding import PartitionSpec as P

MESH = pl.DeviceIdType.MESH
NXC, NZ = 4, 8


def layers_kernel(w_hbm, feat, meta, bias, out, inb, outb, wbuf, act, work, ybuf, r1, r2, zr, metav, colv, metas, cols,
                  wl_sem, ws_sem, wr_sem, ms_sem, mr_sem, cs_sem, cr_sem, loc_sem,
                  in_s, in_r, out_s, out_r, ag_s, ag_r, xs_sem, x1_r, x2_r, zs_sem, z_r):
    f32, bf16 = jnp.float32, jnp.bfloat16
    nx, ny, im = lax.axis_index("nx"), lax.axis_index("ny"), lax.axis_index("img")
    x, c = nx // 2, nx % 2
    yl, z = ny // NZ, ny % NZ
    me = yl * 2 + c
    plane = x * NZ + z
    layers = act.shape[0] - 1

    def dev(xx, cc, yy, zz, ii):
        return (xx * 2 + cc, yy * NZ + zz, ii)

    partner = dev(x, 1 - c, yl, z, im)
    near = dev(x, c, 1 - yl, z, im)
    im_up = (im + yl) % 2
    im_dn = (im + 1 - yl) % 2
    xp = dev((x + 1) % NXC, c, yl, z, im)
    xm = dev((x + NXC - 1) % NXC, c, yl, z, im)
    zp = dev(x, c, yl, (z + 1) % NZ, im)
    zm = dev(x, c, yl, (z + NZ - 1) % NZ, im)

    def in_plane(j):
        return dev((x + j // NZ) % NXC, c, yl, (z + j) % NZ, im)

    barrier = pltpu.get_barrier_semaphore()

    def greet(d):
        pl.semaphore_signal(barrier, inc=1, device_id=d, device_id_type=MESH)

    flat = nx * (2 * NZ) + ny
    half = 4 * NXC * NZ

    def member(j):
        k = (flat + j) % half
        return k, (k // (2 * NZ), k % (2 * NZ), im)

    def greet_half(j, carry):
        greet(member(j)[1])
        return carry

    for cc in (0, 1):
        greet(dev(x, cc, 1 - yl, z, 1 - im))
    lax.fori_loop(1, half, greet_half, 0)
    pl.semaphore_wait(barrier, 2 + half - 1)

    def remote(src, dst, ss, rs, d):
        return pltpu.make_async_remote_copy(src_ref=src, dst_ref=dst, send_sem=ss, recv_sem=rs,
                                            device_id=d, device_id_type=MESH)

    def w_remote(l, xx, cc, yy, ii, slot):
        first = (xx * 2 + cc) * 2 * NZ + yy * NZ
        return remote(w_hbm.at[l, pl.ds(first, NZ)], wbuf.at[l, me, pl.ds(xx * NZ, NZ)],
                      ws_sem.at[l, slot], wr_sem.at[l, me, xx], dev(x, cc, yy, z, ii))

    def w_copies(l, part):
        i = part
        res = [w_remote(l, 2 * i, 1 - c, yl, im, 2 * i), w_remote(l, 2 * i + 1, 1 - c, yl, im, 2 * i + 1)]
        for cc in (0, 1):
            res.append(w_remote(l, i, cc, 1 - yl, im_up, 4 + 2 * i + cc))
            res.append(w_remote(l, 2 + i, cc, 1 - yl, im_dn, 8 + 2 * i + cc))
        return res

    def w_local(l, xx):
        first = (xx * 2 + c) * 2 * NZ + yl * NZ
        return pltpu.make_async_copy(w_hbm.at[l, pl.ds(first, NZ)], wbuf.at[l, me, pl.ds(xx * NZ, NZ)],
                                     wl_sem.at[l, xx])

    def start_weights(l, part):
        for cp in w_copies(l, part):
            cp.start()
        if part == 0:
            for xx in range(NXC):
                w_local(l, xx).start()

    def wait_weights(l):
        for xx in range(NXC):
            w_local(l, xx).wait()
        for k in range(1, 4):
            src = (me + k) % 4
            for xx in range(NXC):
                remote(w_hbm.at[l, pl.ds(0, NZ)], wbuf.at[l, src, pl.ds(xx * NZ, NZ)],
                       ws_sem.at[l, 0], wr_sem.at[l, src, xx], partner).wait_recv()

    def ag(l, src, slot, d):
        return remote(act.at[l, src], act.at[l, src], ag_s.at[l, slot], ag_r.at[l, slot], d)

    def gather_start(l):
        ag(l, me, 0, near).start()
        ag(l, me, 1, partner).start()

    nb = (1 - yl) * 2 + c

    def gather_finish(l):
        ag(l, nb, 0, near).wait_recv()
        ag(l, nb, 2, partner).start()
        ag(l, yl * 2 + 1 - c, 1, partner).wait_recv()
        ag(l, (1 - yl) * 2 + 1 - c, 2, partner).wait_recv()
        ag(l, me, 0, near).wait_send()
        ag(l, me, 1, partner).wait_send()
        ag(l, nb, 2, partner).wait_send()

    def in_cp(j):
        k, d = member(j)
        return remote(feat.at[k], inb.at[flat], in_s, in_r, d)

    def send_in(j, carry):
        in_cp(j).start()
        return carry

    lax.fori_loop(1, half, send_in, 0)
    inb[flat] = feat[flat]

    metav[me] = meta[pl.ds(0, 8), :]
    colv[plane] = meta[pl.ds(8, 8), :]

    def meta_cp(k, d):
        return remote(meta.at[pl.ds(0, 8)], metav.at[me], ms_sem.at[k], mr_sem.at[k], d)

    def col_cp(j):
        return remote(meta.at[pl.ds(8, 8)], colv.at[plane], cs_sem.at[j], cr_sem.at[j], in_plane(j))

    meta_cp(0, partner).start()
    meta_cp(1, near).start()
    meta_cp(2, dev(x, 1 - c, 1 - yl, z, im)).start()

    def send_col(j, carry):
        col_cp(j).start()
        return carry

    lax.fori_loop(1, NXC * NZ, send_col, 0)
    start_weights(0, 0)
    lot = remote(feat.at[pl.ds(0, half - 1)], inb.at[pl.ds(0, half - 1)], in_s, in_r, partner)
    lot.wait_recv()
    for r in range(4):
        act[0, me, r] = inb[:, r, 0, :].astype(f32).astype(bf16)
    gather_start(0)
    start_weights(0, 1)
    gather_finish(0)
    lot.wait_send()
    for k, d, src in ((0, partner, yl * 2 + 1 - c), (1, near, nb), (2, dev(x, 1 - c, 1 - yl, z, im), (1 - yl) * 2 + 1 - c)):
        remote(meta.at[pl.ds(0, 8)], metav.at[src], ms_sem.at[k], mr_sem.at[k], d).wait_recv()
        meta_cp(k, d).wait_send()

    def wait_col(j, carry):
        frm = ((x + NXC - j // NZ) % NXC) * NZ + (z + NZ - j % NZ) % NZ
        remote(meta.at[pl.ds(8, 8)], colv.at[frm], cs_sem.at[j], cr_sem.at[j], in_plane(j)).wait_recv()
        col_cp(j).wait_send()
        return carry

    lax.fori_loop(1, NXC * NZ, wait_col, 0)
    cp = pltpu.make_async_copy(metav, metas, loc_sem.at[0])
    cp2 = pltpu.make_async_copy(colv, cols, loc_sem.at[1])
    cp.start()
    cp2.start()
    cp.wait()
    cp2.wait()

    za = [(z + 4 - j) % NZ for j in range(4)]
    zb = [(z + NZ - 3 + j) % NZ for j in range(4)]
    x1, x2, x3 = (x + 1) % NXC, (x + 2) % NXC, (x + 3) % NXC

    def layer(l, carry):
        @pl.when(l > 0)
        def _():
            gather_finish(l)

        @pl.when(l < layers - 1)
        def _():
            start_weights(l + 1, 0)
            start_weights(l + 1, 1)

        wait_weights(l)
        for s in range(4):
            work[s] = act[l, s]

        def one(e, carry):
            dest = ((e // NZ) * 2 + c) * 2 * NZ + yl * NZ + e % NZ
            lhs, rhs = [], []
            for s in range(4):
                src = (x * 2 + s % 2) * 2 * NZ + (s // 2) * NZ + z
                row, live, col = metas[s, l, dest], metas[s, 3 + l, dest], cols[e, l, src]
                lhs.append(work[s, row])
                block = wbuf[l, s, e]
                key = jnp.where(live == 1, col, 4)
                rhs.append(jnp.concatenate(
                    [jnp.where(key == k, block, jnp.zeros_like(block)) for k in range(4)], axis=1))
            res = jnp.dot(jnp.concatenate(lhs, axis=1), jnp.concatenate(rhs, axis=0), preferred_element_type=f32)
            for k in range(4):
                ybuf[e // NZ, e % NZ, k] = res[:, k * 128:(k + 1) * 128].astype(bf16)
            return carry

        lax.fori_loop(0, NXC * NZ, one, 0)

        def s1(side, j):
            zz = za[j] if side == 0 else zb[j]
            return remote(ybuf.at[x2, zz], r1.at[l, side, j], xs_sem.at[l, side, j], x1_r.at[l, side, j],
                          xp if side == 0 else xm)

        def s2(side, p):
            zz = za[p] if p < 4 else zb[p - 4]
            return remote(ybuf.at[x1 if side == 0 else x3, zz], r2.at[l, side, p], xs_sem.at[l, side, 4 + p],
                          x2_r.at[l, side, p], xp if side == 0 else xm)

        for j in range(4):
            s1(0, j).start()
            s1(1, j).start()
        for j in range(4):
            s2(0, 4 + j).start()
            s2(1, j).start()
            for side, p in ((0, j), (1, 4 + j)):
                s1(side, j).wait_recv()
                xx, zz = (x1, za[j]) if side == 0 else (x3, zb[j])
                ybuf[xx, zz] = (ybuf[xx, zz].astype(f32) + r1[l, side, j].astype(f32)).astype(bf16)
                s2(side, p).start()

        def zcp(side, o):
            d, slot = (zp, 4 - o) if side == 0 else (zm, 4 + 3 + o)
            zz = (z + o + NZ) % NZ
            return remote(ybuf.at[x, zz], zr.at[l, slot], zs_sem.at[l, slot], z_r.at[l, slot], d)

        def total(p, zz):
            s2(0, p).wait_recv()
            s2(1, p).wait_recv()
            return (ybuf[x, zz].astype(f32) + r2[l, 0, p].astype(f32)) + r2[l, 1, p].astype(f32)

        for j in range(4):
            acc = total(j, za[j])
            if j > 0:
                zcp(0, 5 - j).wait_recv()
                acc = acc + zr[l, j - 1].astype(f32)
            ybuf[x, za[j]] = acc.astype(bf16)
            zcp(0, 4 - j).start()
            acc = total(4 + j, zb[j])
            if j > 0:
                zcp(1, -4 + j).wait_recv()
                acc = acc + zr[l, 4 + j - 1].astype(f32)
            if j < 3:
                ybuf[x, zb[j]] = acc.astype(bf16)
                zcp(1, -3 + j).start()
        zcp(0, 1).wait_recv()
        pre = acc + zr[l, 3].astype(f32) + bias[l]
        act[l + 1, me] = jnp.maximum(pre, 0.0).astype(bf16)

        @pl.when(l < layers - 1)
        def _():
            gather_start(l + 1)

        for side in (0, 1):
            for j in range(4):
                s1(side, j).wait_send()
            for p in range(8):
                s2(side, p).wait_send()
        for j in range(4):
            zcp(0, 4 - j).wait_send()
            if j < 3:
                zcp(1, -3 + j).wait_send()
        for cp in w_copies(l, 0) + w_copies(l, 1):
            cp.wait_send()
        return carry

    lax.fori_loop(0, layers, layer, 0)
    for r in range(4):
        outb[:, r, 0, :] = act[layers, me, r]

    def send_out(j, carry):
        k, d = member(j)
        remote(outb.at[k], out.at[flat], out_s, out_r, d).start()
        return carry

    lax.fori_loop(1, half, send_out, 0)
    out[flat] = outb[flat]
    lot = remote(outb.at[pl.ds(0, half - 1)], out.at[pl.ds(0, half - 1)], out_s, out_r, partner)
    lot.wait_recv()
    lot.wait_send()


def run_layers(w, feat, meta, bias):
    layers, half = w.shape[0], feat.shape[0]
    bf16, DMA = jnp.bfloat16, pltpu.SemaphoreType.DMA
    piece = (4, half, 128)
    vm = pl.BlockSpec(memory_space=pltpu.VMEM)
    return pl.pallas_call(
        layers_kernel,
        out_shape=jax.ShapeDtypeStruct(feat.shape, bf16),
        in_specs=[pl.BlockSpec(memory_space=pl.ANY), vm, vm, vm],
        out_specs=vm,
        scratch_shapes=[
            pltpu.VMEM(feat.shape, bf16),
            pltpu.VMEM(feat.shape, bf16),
            pltpu.VMEM((layers, 4, NXC * NZ, 128, 128), bf16),
            pltpu.VMEM((layers + 1, 4) + piece, bf16),
            pltpu.VMEM((4,) + piece, bf16),
            pltpu.VMEM((NXC, NZ) + piece, bf16),
            pltpu.VMEM((layers, 2, 4) + piece, bf16),
            pltpu.VMEM((layers, 2, 8) + piece, bf16),
            pltpu.VMEM((layers, 7) + piece, bf16),
            pltpu.VMEM((4, 8, 128), jnp.int32),
            pltpu.VMEM((NXC * NZ, 8, 128), jnp.int32),
            pltpu.SMEM((4, 8, 128), jnp.int32),
            pltpu.SMEM((NXC * NZ, 8, 128), jnp.int32),
            DMA((layers, 4)), DMA((layers, 12)), DMA((layers, 4, 4)),
            DMA((3,)), DMA((3,)), DMA((NXC * NZ,)), DMA((NXC * NZ,)), DMA((2,)),
            DMA, DMA, DMA, DMA,
            DMA((layers, 3)), DMA((layers, 3)),
            DMA((layers, 2, 12)), DMA((layers, 2, 4)), DMA((layers, 2, 8)),
            DMA((layers, 7)), DMA((layers, 7)),
        ],
        compiler_params=pltpu.CompilerParams(
            collective_id=0, has_side_effects=True, vmem_limit_bytes=56 * 1024 * 1024),
    )(w, feat, meta, bias)


def local(features, link_weight, link_row, link_col, link_live, bias):
    two = jnp.zeros((2, 128), jnp.int32)
    five = jnp.zeros((5, 128), jnp.int32)
    meta = jnp.concatenate([link_row[:, 0], link_live[:, 0], two, link_col[:, :, 0], five], axis=0)
    res = run_layers(link_weight[:, 0], features.reshape(128, 4, 1, 128), meta,
                     bias.reshape(bias.shape[0], 4, 1, 128))
    return res.reshape(features.shape)


def solution(mesh):
    placed = (
        P(("nx", "ny", "img"), None),
        P(None, ("nx", "ny"), None, None, None),
        P(None, ("nx", "ny"), None),
        P(None, None, ("nx", "ny")),
        P(None, ("nx", "ny"), None),
        P(None, ("nx", "ny")),
    )
    return jax.shard_map(
        local, mesh=mesh, in_specs=placed, out_specs=P(("nx", "ny", "img"), None), check_vma=False
    )
```

```python
import jax
import jax.numpy as jnp
from jax import lax
from jax.experimental import pallas as pl
from jax.experimental.pallas import tpu as pltpu
from jax.sharding import PartitionSpec as P

MESH = pl.DeviceIdType.MESH
NXC, NZ = 4, 8
NY = 2 * NZ
HALF = 2 * NXC * NY
HA = 64
HB = HALF - HA
UP = (0, 1, 3, 5)
DOWN = (0, 2, 4, 6)


def bslot(side, level, role):
    return side * 2 + role % 2 if level == 0 else 4 + ((level - 1) * 2 + side) * 4 + role


def layers_kernel(w_hbm, feat, meta, bias, out, inb, outb, wbuf, acta, actb, work,
                  yab, yaf, sa, saz, ybf, sbz, sbx, ra, zra, zrb, rb, metav, colv, metas, cols,
                  wl_sem, ws_sem, wr_sem, ms_sem, mr_sem, cs_sem, cr_sem, loc_sem,
                  in_s, in_r, out_s, out_r, ag_s, ag_r,
                  sa_sem, ra_sem, sza_sem, rza_sem, szb_sem, rzb_sem, sxb_sem, rxb_sem):
    f32, bf16 = jnp.float32, jnp.bfloat16
    nx, ny, im = lax.axis_index("nx"), lax.axis_index("ny"), lax.axis_index("img")
    x, c = nx // 2, nx % 2
    yl, z = ny // NZ, ny % NZ
    me = yl * 2 + c
    plane = x * NZ + z
    flat = nx * NY + ny
    layers = wbuf.shape[0]

    def dev(xx, cc, yy, zz, ii):
        return (xx * 2 + cc, yy * NZ + zz, ii)

    partner = dev(x, 1 - c, yl, z, im)
    near = dev(x, c, 1 - yl, z, im)
    diag = dev(x, 1 - c, 1 - yl, z, im)
    im_up = (im + yl) % 2
    im_dn = (im + 1 - yl) % 2
    x1, x2, x3 = (x + 1) % NXC, (x + 2) % NXC, (x + 3) % NXC
    xp, xm = dev(x1, c, yl, z, im), dev(x3, c, yl, z, im)
    zp = dev(x, c, yl, (z + 1) % NZ, im)
    zm = dev(x, c, yl, (z + NZ - 1) % NZ, im)

    def col_z(k):
        far = 4 - (k + 1) // 2
        return (z + NZ + jnp.where(k % 2 == 1, far, -far)) % NZ

    def for_half(fn):
        for b in range(1, NY):
            fn(nx * NY + (ny + b) % NY, (nx, (ny + b) % NY, im))

        def rows(a, carry):
            n = (nx + a) % (2 * NXC)
            for b in range(NY):
                fn(n * NY + (ny + b) % NY, (n, (ny + b) % NY, im))
            return carry

        lax.fori_loop(1, 2 * NXC, rows, 0)

    def for_plane(fn):
        def step(j, carry):
            fn(j, dev((x + j // NZ) % NXC, c, yl, (z + j) % NZ, im))
            return carry

        lax.fori_loop(1, NXC * NZ, step, 0)

    def remote(src, dst, ss, rs, d):
        return pltpu.make_async_remote_copy(src_ref=src, dst_ref=dst, send_sem=ss, recv_sem=rs,
                                            device_id=d, device_id_type=MESH)

    barrier = pltpu.get_barrier_semaphore()

    def greet(k, d):
        pl.semaphore_signal(barrier, inc=1, device_id=d, device_id_type=MESH)

    for cc in (0, 1):
        greet(0, dev(x, cc, 1 - yl, z, 1 - im))
    for_half(greet)
    pl.semaphore_wait(barrier, 2 + HALF - 1)

    for_half(lambda k, d: remote(feat.at[k], inb.at[flat], in_s, in_r, d).start())

    metav[me] = meta[pl.ds(0, 8), :]
    colv[plane] = meta[pl.ds(8, 8), :]

    def meta_cp(k, d):
        return remote(meta.at[pl.ds(0, 8)], metav.at[me], ms_sem.at[k], mr_sem.at[k], d)

    group = ((0, partner, yl * 2 + 1 - c), (1, near, (1 - yl) * 2 + c), (2, diag, (1 - yl) * 2 + 1 - c))
    for k, d, _ in group:
        meta_cp(k, d).start()
    for_plane(lambda j, d: remote(meta.at[pl.ds(8, 8)], colv.at[plane], cs_sem, cr_sem, d).start())

    def start_weights(l, lo, hi):
        def step(k, carry):
            zz = col_z(k)

            def send(x0, n, cc, yy, ii):
                remote(w_hbm.at[l, pl.ds(x0, n), cc, yy, zz], wbuf.at[l, me, k, pl.ds(x0, n)],
                       ws_sem.at[l], wr_sem.at[l, k], dev(x, cc, yy, z, ii)).start()

            for cc in (0, 1):
                send(0, 2, cc, 1 - yl, im_up)
                send(2, 2, cc, 1 - yl, im_dn)
            send(0, 4, 1 - c, yl, im)
            pltpu.make_async_copy(w_hbm.at[l, :, c, yl, zz], wbuf.at[l, me, k], wl_sem.at[l, k]).start()
            return carry

        lax.fori_loop(lo, hi, step, 0)

    def wait_weights(l, k):
        pltpu.make_async_copy(w_hbm.at[l, :, c, yl, 0], wbuf.at[l, me, k], wl_sem.at[l, k]).wait()
        three = wbuf.at[l, pl.ds(0, 3), k]
        remote(three, three, ws_sem.at[l], wr_sem.at[l, k], partner).wait_recv()

    acts = (acta, actb)

    def ag(l, st, src, slot, d):
        ref = acts[st].at[l, src]
        return remote(ref, ref, ag_s.at[l, st, slot], ag_r.at[l, st, slot], d)

    def gather_start(l, st):
        ag(l, st, me, 0, near).start()
        ag(l, st, me, 1, partner).start()

    def gather_finish(l):
        for st in (0, 1):
            ag(l, st, (1 - yl) * 2 + c, 0, near).wait_recv()
            ag(l, st, (1 - yl) * 2 + c, 2, partner).start()
        for st in (0, 1):
            ag(l, st, yl * 2 + 1 - c, 1, partner).wait_recv()
            ag(l, st, (1 - yl) * 2 + 1 - c, 2, partner).wait_recv()

    def gather_sent(l):
        for st in (0, 1):
            ag(l, st, me, 0, near).wait_send()
            ag(l, st, me, 1, partner).wait_send()
            ag(l, st, me, 2, partner).wait_send()

    start_weights(0, 0, 2)
    for k, d, src in group:
        remote(meta.at[pl.ds(0, 8)], metav.at[src], ms_sem.at[k], mr_sem.at[k], d).wait_recv()
        meta_cp(k, d).wait_send()
    lot = remote(colv.at[pl.ds(0, NXC * NZ - 1)], colv.at[pl.ds(0, NXC * NZ - 1)], cs_sem, cr_sem, partner)
    lot.wait_recv()
    lot.wait_send()
    tables = (pltpu.make_async_copy(metav, metas, loc_sem.at[0]), pltpu.make_async_copy(colv, cols, loc_sem.at[1]))
    for cp in tables:
        cp.start()
    inb[flat] = feat[flat]
    lot = remote(feat.at[pl.ds(0, HALF - 1)], inb.at[pl.ds(0, HALF - 1)], in_s, in_r, partner)
    lot.wait_recv()
    for r in range(4):
        rows = inb[:, r, 0, :].astype(f32).astype(bf16)
        acta[0, me, r] = rows[:HA]
        actb[0, me, r] = rows[HA:]
    gather_start(0, 0)
    gather_start(0, 1)
    lot.wait_send()
    for cp in tables:
        cp.wait()

    def layer(l, carry):
        @pl.when(l == 0)
        def _():
            start_weights(l, 2, 8)

        @pl.when(l > 0)
        def _():
            start_weights(l, 6, 8)

        gather_finish(l)

        @pl.when(l < layers - 1)
        def _():
            start_weights(l + 1, 0, 6)

        for s in range(4):
            work[s, :, pl.ds(0, HA)] = acta[l, s]
            work[s, :, pl.ds(HA, HB)] = actb[l, s]

        def xa(k, kind, src, d):
            return remote(src, ra.at[l, kind, k], sa_sem.at[l], ra_sem.at[l, kind, k], d)

        def zb(side, level, role):
            n = bslot(side, level, role)
            return remote(sbz.at[n], zrb.at[l, n], szb_sem.at[l], rzb_sem.at[l, n], zm if side else zp)

        def zb_now(side, level, k, role):
            sbz[bslot(side, level, role)] = ybf[k, role].astype(bf16)
            zb(side, level, role).start()

        def column(k, carry):
            wait_weights(l, k)
            zz = col_z(k)
            towards = jnp.logical_or(k % 2 == 1, k == 0)
            pick = jnp.where(towards, 1, 0)
            xs = (x2, jnp.where(towards, x1, x3), jnp.where(towards, x3, x1), x)
            roles = (0, 2 - pick, 1 + pick, 3)
            for n in range(4):
                dest = (xs[n] * 2 + c) * NY + yl * NZ + zz
                lhs, rhs = [], []
                for s in range(4):
                    src = (x * 2 + s % 2) * NY + (s // 2) * NZ + z
                    row, live, col = metas[s, l, dest], metas[s, 3 + l, dest], cols[xs[n] * NZ + zz, l, src]
                    lhs.append(work[s, row])
                    block = wbuf[l, s, k, xs[n]]
                    key = jnp.where(live == 1, col, 4)
                    rhs.append(jnp.concatenate(
                        [jnp.where(key == q, block, jnp.zeros_like(block)) for q in range(4)], axis=1))
                res = jnp.dot(jnp.concatenate(lhs, axis=1), jnp.concatenate(rhs, axis=0), preferred_element_type=f32)
                for q in range(4):
                    part = res[:, q * 128:(q + 1) * 128]
                    ybf[k, roles[n], q] = part[HA:]
                    if n == 0:
                        yab[k, 0, q] = part[:HA].astype(bf16)
                    elif n == 2:
                        yab[k, 1, q] = part[:HA].astype(bf16)
                    else:
                        yaf[k, n // 2, q] = part[:HA]
            first = tuple(jnp.where(towards, p, m) for p, m in zip(xp, xm))
            xa(k, 0, yab.at[k, 0], first).start()

            @pl.when(k == 0)
            def _():
                for role in range(4):
                    zb_now(role // 2, 0, 0, role)

            @pl.when(k == 1)
            def _():
                for role in (2, 3):
                    zb_now(0, 1, 1, role)

            @pl.when(k == 2)
            def _():
                for role in (0, 1):
                    zb_now(1, 1, 2, role)

            @pl.when(k % 2 == 0)
            def _():
                @pl.when(k < 3)
                def _():
                    other = tuple(jnp.where(towards, m, p) for p, m in zip(xp, xm))
                    xa(k, 1, yab.at[k, 1], other).start()

            return carry

        lax.fori_loop(0, NZ, column, 0)

        def a_plus(k):
            return k % 2 == 1 or k == 0

        def a_imm(k):
            xa(k, 1, yab.at[k, 1], xm if a_plus(k) else xp).start()

        def a_acc(k):
            xa(k, 0, yab.at[k, 0], xp).wait_recv()
            sa[k] = (yaf[k, 0] + ra[l, 0, k].astype(f32)).astype(bf16)
            xa(k, 2, sa.at[k], xp if a_plus(k) else xm).start()

        def za(k):
            return remote(saz.at[k], zra.at[l, k], sza_sem.at[l], rza_sem.at[l, k], zp if a_plus(k) else zm)

        def a_total(k):
            for kind in (1, 2):
                xa(k, kind, sa.at[k], xp).wait_recv()
            acc = (yaf[k, 1] + ra[l, 1, k].astype(f32)) + ra[l, 2, k].astype(f32)
            for chain in (UP, DOWN[1:]):
                seq = chain + (7,)
                for p in range(1, len(seq)):
                    if seq[p] == k:
                        za(seq[p - 1]).wait_recv()
                        acc = acc + zra[l, seq[p - 1]].astype(f32)
            if k < 7:
                saz[k] = acc.astype(bf16)
                za(k).start()
            else:
                acta[l + 1, me] = jnp.maximum(acc + bias[l], 0.0).astype(bf16)

        def b_step(level, role):
            for side, chain in ((0, UP), (1, DOWN)):
                if level == 1 and role // 2 != side:
                    continue
                zb(side, level - 1, role).wait_recv()
                n = bslot(side, level, role)
                sbz[n] = (ybf[chain[level], role] + zrb[l, bslot(side, level - 1, role)].astype(f32)).astype(bf16)
                zb(side, level, role).start()

        def xb(n, d):
            return remote(sbx.at[n], rb.at[l, n], sxb_sem.at[l], rxb_sem.at[l, n], d)

        def b_sum(role):
            for side in (0, 1):
                zb(side, 3, role).wait_recv()
            return ybf[7, role] + zrb[l, bslot(0, 3, role)].astype(f32) + zrb[l, bslot(1, 3, role)].astype(f32)

        def b_far():
            acc = b_sum(0)
            sbx[0] = acc[0:2].astype(bf16)
            xb(0, xp).start()
            sbx[1] = acc[2:4].astype(bf16)
            xb(1, xm).start()

        def b_next(side):
            acc = b_sum(1 + side)
            lo, hi = (0, 2) if side == 0 else (2, 0)
            d = xm if side else xp
            sbx[3 + 2 * side] = acc[hi:hi + 2].astype(bf16)
            xb(3 + 2 * side, d).start()
            xb(side, d).wait_recv()
            sbx[2 + 2 * side] = (acc[lo:lo + 2] + rb[l, side].astype(f32)).astype(bf16)
            xb(2 + 2 * side, d).start()

        def b_final():
            ybf[7, 3] = b_sum(3)
            for n in range(2, 6):
                xb(n, xp).wait_recv()
            for lo, up, dn in ((0, 2, 5), (2, 3, 4)):
                acc = ybf[7, 3, lo:lo + 2] + rb[l, up].astype(f32) + rb[l, dn].astype(f32)
                actb[l + 1, me, lo:lo + 2] = jnp.maximum(acc + bias[l, lo:lo + 2], 0.0).astype(bf16)

        a_acc(0)
        a_acc(2)
        for role in (0, 2, 1, 3):
            b_step(1, role)
        for k in (1, 4, 3):
            a_imm(k)
            a_acc(k)
        a_imm(6)
        b_step(2, 0)
        a_acc(6)
        a_imm(5)
        a_acc(5)
        b_step(2, 1)
        a_imm(7)
        a_acc(7)
        b_step(2, 2)
        a_total(0)
        b_step(2, 3)
        a_total(1)
        a_total(2)
        b_step(3, 0)
        b_step(3, 1)
        a_total(3)
        b_step(3, 2)
        a_total(4)
        b_step(3, 3)
        b_far()
        a_total(5)
        b_next(0)
        b_next(1)
        a_total(6)
        a_total(7)

        @pl.when(l < layers - 1)
        def _():
            gather_start(l + 1, 0)

        b_final()

        @pl.when(l < layers - 1)
        def _():
            gather_start(l + 1, 1)

        gather_sent(l)
        for ref, sem in ((ra, sa_sem), (zra, sza_sem), (zrb, szb_sem), (rb, sxb_sem)):
            remote(ref.at[l], ref.at[l], sem.at[l], ra_sem.at[l, 0, 0], partner).wait_send()
        sent = wbuf.at[l, pl.ds(0, 3)]
        remote(sent, sent, ws_sem.at[l], wr_sem.at[l, 0], partner).wait_send()
        return carry

    lax.fori_loop(0, layers, layer, 0)

    for r in range(4):
        outb[pl.ds(0, HA), r, 0, :] = acta[layers, me, r]
        outb[pl.ds(HA, HB), r, 0, :] = actb[layers, me, r]
    for_half(lambda k, d: remote(outb.at[k], out.at[flat], out_s, out_r, d).start())
    out[flat] = outb[flat]
    lot = remote(outb.at[pl.ds(0, HALF - 1)], out.at[pl.ds(0, HALF - 1)], out_s, out_r, partner)
    lot.wait_recv()
    lot.wait_send()


def run_layers(w, feat, meta, bias):
    layers = w.shape[0]
    bf16, f32, DMA = jnp.bfloat16, jnp.float32, pltpu.SemaphoreType.DMA
    pa, pb, hb = (4, HA, 128), (4, HB, 128), (2, HB, 128)
    vm = pl.BlockSpec(memory_space=pltpu.VMEM)
    return pl.pallas_call(
        layers_kernel,
        out_shape=jax.ShapeDtypeStruct(feat.shape, bf16),
        in_specs=[pl.BlockSpec(memory_space=pl.ANY), vm, vm, vm],
        out_specs=vm,
        scratch_shapes=[
            pltpu.VMEM(feat.shape, bf16),
            pltpu.VMEM(feat.shape, bf16),
            pltpu.VMEM((layers, 4, NZ, NXC, 128, 128), bf16),
            pltpu.VMEM((layers + 1, 4) + pa, bf16),
            pltpu.VMEM((layers + 1, 4) + pb, bf16),
            pltpu.VMEM((4, 4, HALF, 128), bf16),
            pltpu.VMEM((NZ, 2) + pa, bf16),
            pltpu.VMEM((NZ, 2) + pa, f32),
            pltpu.VMEM((NZ,) + pa, bf16),
            pltpu.VMEM((NZ - 1,) + pa, bf16),
            pltpu.VMEM((NZ, 4) + pb, f32),
            pltpu.VMEM((28,) + pb, bf16),
            pltpu.VMEM((6,) + hb, bf16),
            pltpu.VMEM((layers, 3, NZ) + pa, bf16),
            pltpu.VMEM((layers, NZ - 1) + pa, bf16),
            pltpu.VMEM((layers, 28) + pb, bf16),
            pltpu.VMEM((layers, 6) + hb, bf16),
            pltpu.VMEM((4, 8, 128), jnp.int32),
            pltpu.VMEM((NXC * NZ, 8, 128), jnp.int32),
            pltpu.SMEM((4, 8, 128), jnp.int32),
            pltpu.SMEM((NXC * NZ, 8, 128), jnp.int32),
            DMA((layers, NZ)), DMA((layers,)), DMA((layers, NZ)),
            DMA((3,)), DMA((3,)), DMA, DMA, DMA((2,)),
            DMA, DMA, DMA, DMA,
            DMA((layers, 2, 3)), DMA((layers, 2, 3)),
            DMA((layers,)), DMA((layers, 3, NZ)),
            DMA((layers,)), DMA((layers, NZ - 1)),
            DMA((layers,)), DMA((layers, 28)),
            DMA((layers,)), DMA((layers, 6)),
        ],
        compiler_params=pltpu.CompilerParams(
            collective_id=0, has_side_effects=True, vmem_limit_bytes=60 * 1024 * 1024),
    )(w, feat, meta, bias)


def local(features, link_weight, link_row, link_col, link_live, bias):
    two = jnp.zeros((2, 128), jnp.int32)
    five = jnp.zeros((5, 128), jnp.int32)
    meta = jnp.concatenate([link_row[:, 0], link_live[:, 0], two, link_col[:, :, 0], five], axis=0)
    layers = bias.shape[0]
    res = run_layers(link_weight.reshape(layers, NXC, 2, 2, NZ, 128, 128), features.reshape(HALF, 4, 1, 128), meta,
                     bias.reshape(layers, 4, 1, 128))
    return res.reshape(features.shape)


def solution(mesh):
    placed = (
        P(("nx", "ny", "img"), None),
        P(None, ("nx", "ny"), None, None, None),
        P(None, ("nx", "ny"), None),
        P(None, None, ("nx", "ny")),
        P(None, ("nx", "ny"), None),
        P(None, ("nx", "ny")),
    )
    return jax.shard_map(
        local, mesh=mesh, in_specs=placed, out_specs=P(("nx", "ny", "img"), None), check_vma=False
    )
```

```python
import jax
import jax.numpy as jnp
from jax import lax
from jax.experimental import pallas as pl
from jax.experimental.pallas import tpu as pltpu
from jax.sharding import PartitionSpec as P

MESH = pl.DeviceIdType.MESH
NXC, NZ = 4, 8
NY = 2 * NZ
HALF = 2 * NXC * NY
HA = 64
HB = HALF - HA
UP = (0, 1, 3, 5)
DOWN = (0, 2, 4, 6)


def bslot(side, level, role):
    return side * 2 + role % 2 if level == 0 else 4 + ((level - 1) * 2 + side) * 4 + role


def layers_kernel(w_hbm, feat, row_in, live_in, col_in, bias, out, pack, meta, biasv, inb, outb, wbuf, acta, actb, work,
                  yab, yaf, sa, saz, ybf, sbz, sbx, ra, zra, zrb, rb, metav, colv, metas, cols,
                  wl_sem, ws_sem, wr_sem, ms_sem, mr_sem, cs_sem, cr_sem, loc_sem,
                  in_s, in_r, out_s, out_r, ag_s, ag_r,
                  sa_sem, ra_sem, sza_sem, rza_sem, szb_sem, rzb_sem, sxb_sem, rxb_sem):
    f32, bf16 = jnp.float32, jnp.bfloat16
    nx, ny, im = lax.axis_index("nx"), lax.axis_index("ny"), lax.axis_index("img")
    x, c = nx // 2, nx % 2
    yl, z = ny // NZ, ny % NZ
    me = yl * 2 + c
    plane = x * NZ + z
    flat = nx * NY + ny
    layers = wbuf.shape[0]

    def dev(xx, cc, yy, zz, ii):
        return (xx * 2 + cc, yy * NZ + zz, ii)

    partner = dev(x, 1 - c, yl, z, im)
    near = dev(x, c, 1 - yl, z, im)
    diag = dev(x, 1 - c, 1 - yl, z, im)
    im_up = (im + yl) % 2
    im_dn = (im + 1 - yl) % 2
    x1, x2, x3 = (x + 1) % NXC, (x + 2) % NXC, (x + 3) % NXC
    xp, xm = dev(x1, c, yl, z, im), dev(x3, c, yl, z, im)
    zp = dev(x, c, yl, (z + 1) % NZ, im)
    zm = dev(x, c, yl, (z + NZ - 1) % NZ, im)

    def col_z(k):
        far = 4 - (k + 1) // 2
        return (z + NZ + jnp.where(k % 2 == 1, far, -far)) % NZ

    def for_half(fn):
        for b in range(1, NY):
            fn(nx * NY + (ny + b) % NY, (nx, (ny + b) % NY, im))

        def rows(a, carry):
            n = (nx + a) % (2 * NXC)
            for b in range(NY):
                fn(n * NY + (ny + b) % NY, (n, (ny + b) % NY, im))
            return carry

        lax.fori_loop(1, 2 * NXC, rows, 0)

    def for_plane(fn):
        def step(j, carry):
            fn(j, dev((x + j // NZ) % NXC, c, yl, (z + j) % NZ, im))
            return carry

        lax.fori_loop(1, NXC * NZ, step, 0)

    def remote(src, dst, ss, rs, d):
        return pltpu.make_async_remote_copy(src_ref=src, dst_ref=dst, send_sem=ss, recv_sem=rs,
                                            device_id=d, device_id_type=MESH)

    for r in range(4):
        pack[:, r, :] = feat[:, r, 0, :]
    for i in range(row_in.shape[0]):
        meta[i, :] = row_in[i, 0, :]
        meta[3 + i, :] = live_in[i, 0, :]
        meta[8 + i, :] = col_in[i, 0, :]
        for r in range(4):
            biasv[i, r, 0, :] = bias[i, r * 128:(r + 1) * 128]

    barrier = pltpu.get_barrier_semaphore()

    def greet(k, d):
        pl.semaphore_signal(barrier, inc=1, device_id=d, device_id_type=MESH)

    for cc in (0, 1):
        greet(0, dev(x, cc, 1 - yl, z, 1 - im))
    for_half(greet)
    pl.semaphore_wait(barrier, 2 + HALF - 1)

    for_half(lambda k, d: remote(pack.at[k], inb.at[flat], in_s, in_r, d).start())

    metav[me] = meta[pl.ds(0, 8), :]
    colv[plane] = meta[pl.ds(8, 8), :]

    def meta_cp(k, d):
        return remote(meta.at[pl.ds(0, 8)], metav.at[me], ms_sem.at[k], mr_sem.at[k], d)

    group = ((0, partner, yl * 2 + 1 - c), (1, near, (1 - yl) * 2 + c), (2, diag, (1 - yl) * 2 + 1 - c))
    for k, d, _ in group:
        meta_cp(k, d).start()
    for_plane(lambda j, d: remote(meta.at[pl.ds(8, 8)], colv.at[plane], cs_sem, cr_sem, d).start())

    def start_weights(l, lo, hi):
        def step(k, carry):
            zz = col_z(k)

            def send(x0, n, cc, yy, ii):
                remote(w_hbm.at[l, pl.ds(x0, n), cc, yy, zz], wbuf.at[l, me, k, pl.ds(x0, n)],
                       ws_sem.at[l], wr_sem.at[l, k], dev(x, cc, yy, z, ii)).start()

            for cc in (0, 1):
                send(0, 2, cc, 1 - yl, im_up)
                send(2, 2, cc, 1 - yl, im_dn)
            send(0, 4, 1 - c, yl, im)
            pltpu.make_async_copy(w_hbm.at[l, :, c, yl, zz], wbuf.at[l, me, k], wl_sem.at[l, k]).start()
            return carry

        lax.fori_loop(lo, hi, step, 0)

    def wait_weights(l, k):
        pltpu.make_async_copy(w_hbm.at[l, :, c, yl, 0], wbuf.at[l, me, k], wl_sem.at[l, k]).wait()
        three = wbuf.at[l, pl.ds(0, 3), k]
        remote(three, three, ws_sem.at[l], wr_sem.at[l, k], partner).wait_recv()

    acts = (acta, actb)

    def ag(l, st, src, slot, d):
        ref = acts[st].at[l, src]
        return remote(ref, ref, ag_s.at[l, st, slot], ag_r.at[l, st, slot], d)

    def gather_start(l, st):
        ag(l, st, me, 0, near).start()
        ag(l, st, me, 1, partner).start()

    def gather_finish(l):
        for st in (0, 1):
            ag(l, st, (1 - yl) * 2 + c, 0, near).wait_recv()
            ag(l, st, (1 - yl) * 2 + c, 2, partner).start()
        for st in (0, 1):
            ag(l, st, yl * 2 + 1 - c, 1, partner).wait_recv()
            ag(l, st, (1 - yl) * 2 + 1 - c, 2, partner).wait_recv()

    def gather_sent(l):
        for st in (0, 1):
            ag(l, st, me, 0, near).wait_send()
            ag(l, st, me, 1, partner).wait_send()
            ag(l, st, me, 2, partner).wait_send()

    start_weights(0, 0, 4)
    for k, d, src in group:
        remote(meta.at[pl.ds(0, 8)], metav.at[src], ms_sem.at[k], mr_sem.at[k], d).wait_recv()
        meta_cp(k, d).wait_send()
    lot = remote(colv.at[pl.ds(0, NXC * NZ - 1)], colv.at[pl.ds(0, NXC * NZ - 1)], cs_sem, cr_sem, partner)
    lot.wait_recv()
    lot.wait_send()
    tables = (pltpu.make_async_copy(metav, metas, loc_sem.at[0]), pltpu.make_async_copy(colv, cols, loc_sem.at[1]))
    for cp in tables:
        cp.start()
    inb[flat] = pack[flat]
    lot = remote(pack.at[pl.ds(0, HALF - 1)], inb.at[pl.ds(0, HALF - 1)], in_s, in_r, partner)
    lot.wait_recv()
    for r in range(4):
        rows = inb[:, r, :]
        acta[0, me, r] = rows[:HA]
        actb[0, me, r] = rows[HA:]
    gather_start(0, 0)
    gather_start(0, 1)
    lot.wait_send()
    for cp in tables:
        cp.wait()

    def bias_of(l, lo, n):
        return biasv[l, lo:lo + n]

    def layer(l, carry):
        @pl.when(l == 0)
        def _():
            start_weights(l, 4, 8)

        @pl.when(l > 0)
        def _():
            start_weights(l, 6, 8)

        gather_finish(l)

        @pl.when(l < layers - 1)
        def _():
            start_weights(l + 1, 0, 6)

        for s in range(4):
            work[s, :, pl.ds(0, HA)] = acta[l, s]
            work[s, :, pl.ds(HA, HB)] = actb[l, s]

        def xa(k, kind, src, d):
            return remote(src, ra.at[l, kind, k], sa_sem.at[l], ra_sem.at[l, kind, k], d)

        def zb(side, level, role):
            n = bslot(side, level, role)
            return remote(sbz.at[n], zrb.at[l, n], szb_sem.at[l], rzb_sem.at[l, n], zm if side else zp)

        def zb_now(side, level, k, role):
            sbz[bslot(side, level, role)] = ybf[k, role].astype(bf16)
            zb(side, level, role).start()

        def column(k, carry):
            wait_weights(l, k)
            zz = col_z(k)
            towards = jnp.logical_or(k % 2 == 1, k == 0)
            pick = jnp.where(towards, 1, 0)
            xs = (x2, jnp.where(towards, x1, x3), jnp.where(towards, x3, x1), x)
            roles = (0, 2 - pick, 1 + pick, 3)
            for n in range(4):
                dest = (xs[n] * 2 + c) * NY + yl * NZ + zz
                lhs, rhs = [], []
                for s in range(4):
                    src = (x * 2 + s % 2) * NY + (s // 2) * NZ + z
                    row, live, col = metas[s, l, dest], metas[s, 3 + l, dest], cols[xs[n] * NZ + zz, l, src]
                    lhs.append(work[s, row])
                    block = wbuf[l, s, k, xs[n]]
                    key = jnp.where(live == 1, col, 4)
                    rhs.append(jnp.concatenate(
                        [jnp.where(key == q, block, jnp.zeros_like(block)) for q in range(4)], axis=1))
                res = jnp.dot(jnp.concatenate(lhs, axis=1), jnp.concatenate(rhs, axis=0), preferred_element_type=f32)
                for q in range(4):
                    part = res[:, q * 128:(q + 1) * 128]
                    ybf[k, roles[n], q] = part[HA:]
                    if n == 0:
                        yab[k, 0, q] = part[:HA].astype(bf16)
                    elif n == 2:
                        yab[k, 1, q] = part[:HA].astype(bf16)
                    else:
                        yaf[k, n // 2, q] = part[:HA]
            first = tuple(jnp.where(towards, p, m) for p, m in zip(xp, xm))
            xa(k, 0, yab.at[k, 0], first).start()

            @pl.when(k == 0)
            def _():
                for role in range(4):
                    zb_now(role // 2, 0, 0, role)

            @pl.when(k == 1)
            def _():
                for role in (2, 3):
                    zb_now(0, 1, 1, role)

            @pl.when(k == 2)
            def _():
                for role in (0, 1):
                    zb_now(1, 1, 2, role)

            @pl.when(k % 2 == 0)
            def _():
                @pl.when(k < 3)
                def _():
                    other = tuple(jnp.where(towards, m, p) for p, m in zip(xp, xm))
                    xa(k, 1, yab.at[k, 1], other).start()

            return carry

        lax.fori_loop(0, NZ, column, 0)

        def a_plus(k):
            return k % 2 == 1 or k == 0

        def a_imm(k):
            xa(k, 1, yab.at[k, 1], xm if a_plus(k) else xp).start()

        def a_acc(k):
            xa(k, 0, yab.at[k, 0], xp).wait_recv()
            sa[k] = (yaf[k, 0] + ra[l, 0, k].astype(f32)).astype(bf16)
            xa(k, 2, sa.at[k], xp if a_plus(k) else xm).start()

        def za(k):
            return remote(saz.at[k], zra.at[l, k], sza_sem.at[l], rza_sem.at[l, k], zp if a_plus(k) else zm)

        def a_total(k):
            for kind in (1, 2):
                xa(k, kind, sa.at[k], xp).wait_recv()
            acc = (yaf[k, 1] + ra[l, 1, k].astype(f32)) + ra[l, 2, k].astype(f32)
            for chain in (UP, DOWN[1:]):
                seq = chain + (7,)
                for p in range(1, len(seq)):
                    if seq[p] == k:
                        za(seq[p - 1]).wait_recv()
                        acc = acc + zra[l, seq[p - 1]].astype(f32)
            if k < 7:
                saz[k] = acc.astype(bf16)
                za(k).start()
            else:
                acta[l + 1, me] = jnp.maximum(acc + bias_of(l, 0, 4), 0.0).astype(bf16)

        def b_step(level, role):
            for side, chain in ((0, UP), (1, DOWN)):
                if level == 1 and role // 2 != side:
                    continue
                zb(side, level - 1, role).wait_recv()
                n = bslot(side, level, role)
                sbz[n] = (ybf[chain[level], role] + zrb[l, bslot(side, level - 1, role)].astype(f32)).astype(bf16)
                zb(side, level, role).start()

        def xb(n, d):
            return remote(sbx.at[n], rb.at[l, n], sxb_sem.at[l], rxb_sem.at[l, n], d)

        def b_sum(role):
            for side in (0, 1):
                zb(side, 3, role).wait_recv()
            return ybf[7, role] + zrb[l, bslot(0, 3, role)].astype(f32) + zrb[l, bslot(1, 3, role)].astype(f32)

        def b_far():
            acc = b_sum(0)
            sbx[0] = acc[0:2].astype(bf16)
            xb(0, xp).start()
            sbx[1] = acc[2:4].astype(bf16)
            xb(1, xm).start()

        def b_next(side):
            acc = b_sum(1 + side)
            lo, hi = (0, 2) if side == 0 else (2, 0)
            d = xm if side else xp
            sbx[3 + 2 * side] = acc[hi:hi + 2].astype(bf16)
            xb(3 + 2 * side, d).start()
            xb(side, d).wait_recv()
            sbx[2 + 2 * side] = (acc[lo:lo + 2] + rb[l, side].astype(f32)).astype(bf16)
            xb(2 + 2 * side, d).start()

        def b_final():
            ybf[7, 3] = b_sum(3)
            for n in range(2, 6):
                xb(n, xp).wait_recv()
            for lo, up, dn in ((0, 2, 5), (2, 3, 4)):
                acc = ybf[7, 3, lo:lo + 2] + rb[l, up].astype(f32) + rb[l, dn].astype(f32)
                actb[l + 1, me, lo:lo + 2] = jnp.maximum(acc + bias_of(l, lo, 2), 0.0).astype(bf16)

        a_acc(0)
        a_acc(2)
        for role in (0, 2, 1, 3):
            b_step(1, role)
        for k in (1, 4, 3):
            a_imm(k)
            a_acc(k)
        a_imm(6)
        b_step(2, 0)
        a_acc(6)
        a_imm(5)
        a_acc(5)
        b_step(2, 1)
        a_imm(7)
        a_acc(7)
        b_step(2, 2)
        a_total(0)
        b_step(2, 3)
        a_total(1)
        a_total(2)
        b_step(3, 0)
        b_step(3, 1)
        a_total(3)
        b_step(3, 2)
        a_total(4)
        b_step(3, 3)
        b_far()
        a_total(5)
        b_next(0)
        b_next(1)
        a_total(6)
        a_total(7)

        @pl.when(l < layers - 1)
        def _():
            gather_start(l + 1, 0)

        b_final()

        @pl.when(l < layers - 1)
        def _():
            gather_start(l + 1, 1)

        gather_sent(l)
        for ref, sem in ((ra, sa_sem), (zra, sza_sem), (zrb, szb_sem), (rb, sxb_sem)):
            remote(ref.at[l], ref.at[l], sem.at[l], ra_sem.at[l, 0, 0], partner).wait_send()
        sent = wbuf.at[l, pl.ds(0, 3)]
        remote(sent, sent, ws_sem.at[l], wr_sem.at[l, 0], partner).wait_send()
        return carry

    lax.fori_loop(0, layers, layer, 0)

    for r in range(4):
        outb[pl.ds(0, HA), r, :] = acta[layers, me, r]
        outb[pl.ds(HA, HB), r, :] = actb[layers, me, r]
    for_half(lambda k, d: remote(outb.at[k], out.at[flat], out_s, out_r, d).start())
    out[flat] = outb[flat]
    lot = remote(outb.at[pl.ds(0, HALF - 1)], out.at[pl.ds(0, HALF - 1)], out_s, out_r, partner)
    lot.wait_recv()
    lot.wait_send()


def run_layers(w, feat, row, live, col, bias):
    layers = w.shape[0]
    bf16, f32, DMA = jnp.bfloat16, jnp.float32, pltpu.SemaphoreType.DMA
    pa, pb, hb = (4, HA, 128), (4, HB, 128), (2, HB, 128)
    slabs = (HALF, 4, 128)
    vm = pl.BlockSpec(memory_space=pltpu.VMEM)
    return pl.pallas_call(
        layers_kernel,
        out_shape=jax.ShapeDtypeStruct(slabs, bf16),
        in_specs=[pl.BlockSpec(memory_space=pl.ANY)] + [vm] * 5,
        out_specs=vm,
        scratch_shapes=[
            pltpu.VMEM(slabs, bf16),
            pltpu.VMEM((16, 128), jnp.int32),
            pltpu.VMEM((layers, 4, 1, 128), f32),
            pltpu.VMEM(slabs, bf16),
            pltpu.VMEM(slabs, bf16),
            pltpu.VMEM((layers, 4, NZ, NXC, 128, 128), bf16),
            pltpu.VMEM((layers + 1, 4) + pa, bf16),
            pltpu.VMEM((layers + 1, 4) + pb, bf16),
            pltpu.VMEM((4, 4, HALF, 128), bf16),
            pltpu.VMEM((NZ, 2) + pa, bf16),
            pltpu.VMEM((NZ, 2) + pa, f32),
            pltpu.VMEM((NZ,) + pa, bf16),
            pltpu.VMEM((NZ - 1,) + pa, bf16),
            pltpu.VMEM((NZ, 4) + pb, f32),
            pltpu.VMEM((28,) + pb, bf16),
            pltpu.VMEM((6,) + hb, bf16),
            pltpu.VMEM((layers, 3, NZ) + pa, bf16),
            pltpu.VMEM((layers, NZ - 1) + pa, bf16),
            pltpu.VMEM((layers, 28) + pb, bf16),
            pltpu.VMEM((layers, 6) + hb, bf16),
            pltpu.VMEM((4, 8, 128), jnp.int32),
            pltpu.VMEM((NXC * NZ, 8, 128), jnp.int32),
            pltpu.SMEM((4, 8, 128), jnp.int32),
            pltpu.SMEM((NXC * NZ, 8, 128), jnp.int32),
            DMA((layers, NZ)), DMA((layers,)), DMA((layers, NZ)),
            DMA((3,)), DMA((3,)), DMA, DMA, DMA((2,)),
            DMA, DMA, DMA, DMA,
            DMA((layers, 2, 3)), DMA((layers, 2, 3)),
            DMA((layers,)), DMA((layers, 3, NZ)),
            DMA((layers,)), DMA((layers, NZ - 1)),
            DMA((layers,)), DMA((layers, 28)),
            DMA((layers,)), DMA((layers, 6)),
        ],
        compiler_params=pltpu.CompilerParams(
            collective_id=0, has_side_effects=True, vmem_limit_bytes=60 * 1024 * 1024),
    )(w, feat, row, live, col, bias)


def local(features, link_weight, link_row, link_col, link_live, bias):
    layers = bias.shape[0]
    res = run_layers(link_weight.reshape(layers, NXC, 2, 2, NZ, 128, 128), features.reshape(HALF, 4, 1, 128),
                     link_row, link_live, link_col.transpose(0, 2, 1), bias)
    return res.reshape(features.shape)


def solution(mesh):
    placed = (
        P(("nx", "ny", "img"), None),
        P(None, ("nx", "ny"), None, None, None),
        P(None, ("nx", "ny"), None),
        P(None, None, ("nx", "ny")),
        P(None, ("nx", "ny"), None),
        P(None, ("nx", "ny")),
    )
    return jax.shard_map(
        local, mesh=mesh, in_specs=placed, out_specs=P(("nx", "ny", "img"), None), check_vma=False
    )
```

```python
import jax
import jax.numpy as jnp
from jax import lax
from jax.experimental import pallas as pl
from jax.experimental.pallas import tpu as pltpu
from jax.sharding import PartitionSpec as P

MESH = pl.DeviceIdType.MESH
NXC, NZ = 4, 8
NY = 2 * NZ
HALF = 2 * NXC * NY
LAYERS = 3
STREAMS = ((0, 48), (0, 32), (1, 48))
OFFSET = tuple(sum(m for _, m in STREAMS[:i]) for i in range(len(STREAMS)))
UP = (0, 1, 3, 5)
DOWN = (0, 2, 4, 6)
JOIN = {0: (1, 1), 1: (1, 3), 2: (1, 4), 3: (1, 5), 4: (1, 6), 5: (1, 7), 6: (1, 7)}
FIRST, EARLY = 4, 6
SEGS = (((0,), (1,), (2,), (3,), (4,), (5,), (6,), (7,)), ((0,), (1, 2), (3, 4), (5, 6, 7)))
AGS, FWD, WORK, COL, S1, IM, AC, TO, FIN, B0, B1, B2, B3, BF, BI, BA, BO = range(17)
ORDER = (
    (AGS, 0, 0, 0), (AGS, 0, 2, 0), (AGS, 0, 1, 0), (FWD, 0, 0, 0), (FWD, 0, 2, 0), (WORK, 0, 0, 0), (COL, 0, 0, 0),
    (FWD, 0, 1, 0), (S1, 0, 0, 0), (COL, 0, 0, 1), (S1, 0, 0, 1), (WORK, 0, 2, 0), (COL, 0, 2, 0), (B0, 0, 2, 0),
    (COL, 0, 2, 1), (B0, 0, 2, 1), (COL, 0, 0, 2), (S1, 0, 0, 2), (COL, 0, 0, 3), (IM, 0, 0, 3), (IM, 0, 0, 1),
    (B0, 0, 2, 2), (IM, 0, 0, 2), (COL, 0, 2, 2), (B1, 0, 2, 5), (COL, 0, 0, 4), (AC, 0, 0, 0), (B1, 0, 2, 4),
    (B1, 0, 2, 2), (S1, 0, 0, 3), (B0, 0, 2, 3), (COL, 0, 2, 3), (COL, 0, 2, 4), (B1, 0, 2, 0), (AC, 0, 0, 1),
    (IM, 0, 0, 0), (S1, 0, 0, 4), (IM, 0, 0, 4), (WORK, 0, 1, 0), (COL, 0, 1, 0), (IM, 0, 1, 0), (COL, 0, 1, 1),
    (COL, 0, 0, 5), (S1, 0, 1, 1), (COL, 0, 2, 5), (S1, 0, 1, 0), (AC, 0, 0, 2), (COL, 0, 1, 2), (S1, 0, 1, 2),
    (B2, 0, 2, 2), (B2, 0, 2, 5), (S1, 0, 0, 5), (B1, 0, 2, 1), (COL, 0, 1, 3), (IM, 0, 1, 1), (COL, 0, 1, 4),
    (COL, 0, 1, 5), (COL, 0, 0, 6), (IM, 0, 1, 4), (S1, 0, 1, 3), (TO, 0, 0, 0), (B2, 0, 2, 0), (COL, 0, 2, 6),
    (S1, 0, 0, 6), (AC, 0, 0, 3), (AC, 0, 0, 4), (B2, 0, 2, 4), (COL, 0, 1, 6), (B1, 0, 2, 7), (B1, 0, 2, 3),
    (B1, 0, 2, 6), (IM, 0, 0, 5), (IM, 0, 1, 2), (B3, 0, 2, 2), (B3, 0, 2, 5), (COL, 0, 1, 7), (COL, 0, 0, 7),
    (TO, 0, 0, 2), (AC, 0, 1, 0), (AC, 0, 1, 1), (IM, 0, 1, 7), (AC, 0, 1, 2), (COL, 0, 2, 7), (TO, 0, 0, 1),
    (AC, 0, 0, 5), (IM, 0, 1, 3), (B2, 0, 2, 1), (B3, 0, 2, 4), (IM, 0, 1, 5), (S1, 0, 0, 7), (B3, 0, 2, 0),
    (S1, 0, 1, 6), (B2, 0, 2, 7), (IM, 0, 0, 6), (B2, 0, 2, 3), (S1, 0, 1, 4), (B2, 0, 2, 6), (IM, 0, 0, 7),
    (AC, 0, 1, 3), (TO, 0, 1, 0), (S1, 0, 1, 7), (AC, 0, 0, 6), (TO, 0, 0, 3), (S1, 0, 1, 5), (TO, 0, 1, 2),
    (TO, 0, 0, 4), (IM, 0, 1, 6), (B3, 0, 2, 1), (BF, 0, 2, 0), (AC, 0, 0, 7), (AC, 0, 1, 6), (B3, 0, 2, 7),
    (B3, 0, 2, 3), (AC, 0, 1, 4), (B3, 0, 2, 6), (TO, 0, 1, 1), (AC, 0, 1, 7), (TO, 0, 0, 5), (TO, 0, 0, 6),
    (AC, 0, 1, 5), (BI, 0, 2, 0), (BA, 0, 2, 0), (BO, 0, 2, 0), (TO, 0, 1, 4), (BI, 0, 2, 1), (BA, 0, 2, 1),
    (TO, 0, 1, 3), (FIN, 0, 0, 0), (AGS, 1, 0, 0), (TO, 0, 1, 6), (TO, 0, 1, 5), (FIN, 0, 2, 0), (AGS, 1, 2, 0),
    (FWD, 1, 0, 0), (WORK, 1, 0, 0), (COL, 1, 0, 0), (S1, 1, 0, 0), (COL, 1, 0, 1), (S1, 1, 0, 1), (FWD, 1, 2, 0),
    (S1, 1, 0, 2), (FIN, 0, 1, 0), (AGS, 1, 1, 0), (COL, 1, 0, 2), (IM, 1, 0, 3), (IM, 1, 0, 1), (IM, 1, 0, 2),
    (S1, 1, 0, 3), (IM, 1, 0, 0), (WORK, 1, 2, 0), (COL, 1, 2, 0), (B0, 1, 2, 0), (COL, 1, 2, 1), (AC, 1, 0, 0),
    (B1, 1, 2, 5), (B0, 1, 2, 1), (B0, 1, 2, 2), (COL, 1, 2, 2), (FWD, 1, 1, 0), (AC, 1, 0, 2), (B1, 1, 2, 4),
    (B1, 1, 2, 2), (AC, 1, 0, 1), (S1, 1, 0, 4), (IM, 1, 0, 4), (B1, 1, 2, 3), (B0, 1, 2, 3), (WORK, 1, 1, 0),
    (COL, 1, 1, 0), (IM, 1, 1, 0), (B1, 1, 2, 0), (S1, 1, 1, 0), (COL, 1, 1, 1), (S1, 1, 1, 1), (S1, 1, 1, 2),
    (AC, 1, 0, 3), (B2, 1, 2, 5), (COL, 1, 1, 2), (IM, 1, 1, 4), (TO, 1, 0, 0), (IM, 1, 1, 1), (IM, 1, 1, 3),
    (B1, 1, 2, 1), (S1, 1, 1, 4), (B1, 1, 2, 6), (B2, 1, 2, 2), (IM, 1, 1, 2), (TO, 1, 0, 2), (S1, 1, 1, 3),
    (B2, 1, 2, 4), (B2, 1, 2, 3), (AC, 1, 0, 4), (COL, 1, 0, 3), (AC, 1, 1, 0), (B2, 1, 2, 0), (S1, 1, 0, 6),
    (S1, 1, 0, 5), (AC, 1, 1, 2), (COL, 1, 2, 3), (AC, 1, 1, 1), (TO, 1, 0, 1), (S1, 1, 0, 7), (B3, 1, 2, 5),
    (COL, 1, 1, 3), (IM, 1, 1, 7), (IM, 1, 0, 6), (B3, 1, 2, 2), (S1, 1, 1, 6), (IM, 1, 1, 5), (AC, 1, 1, 4),
    (B2, 1, 2, 6), (B1, 1, 2, 7), (B2, 1, 2, 1), (TO, 1, 0, 4), (IM, 1, 0, 5), (AC, 1, 1, 3), (B3, 1, 2, 3),
    (B3, 1, 2, 4), (S1, 1, 1, 7), (TO, 1, 1, 0), (IM, 1, 0, 7), (IM, 1, 1, 6), (TO, 1, 1, 2), (B3, 1, 2, 0),
    (AC, 1, 0, 6), (AC, 1, 0, 5), (TO, 1, 0, 3), (B3, 1, 2, 6), (AC, 1, 1, 6), (S1, 1, 1, 5), (AC, 1, 0, 7),
    (B2, 1, 2, 7), (B3, 1, 2, 1), (AC, 1, 1, 7), (TO, 1, 1, 1), (TO, 1, 1, 4), (BF, 1, 2, 0), (TO, 1, 0, 6),
    (BI, 1, 2, 1), (TO, 1, 0, 5), (AC, 1, 1, 5), (B3, 1, 2, 7), (BI, 1, 2, 0), (TO, 1, 1, 6), (TO, 1, 1, 3),
    (BA, 1, 2, 1), (BA, 1, 2, 0), (FIN, 1, 0, 0), (AGS, 2, 0, 0), (BO, 1, 2, 0), (TO, 1, 1, 5), (FIN, 1, 2, 0),
    (AGS, 2, 2, 0), (FWD, 2, 0, 0), (FIN, 1, 1, 0), (AGS, 2, 1, 0), (WORK, 2, 0, 0), (COL, 2, 0, 0), (S1, 2, 0, 0),
    (FWD, 2, 2, 0), (COL, 2, 0, 1), (S1, 2, 0, 1), (S1, 2, 0, 2), (COL, 2, 0, 2), (WORK, 2, 2, 0), (COL, 2, 2, 0),
    (B0, 2, 2, 0), (COL, 2, 2, 1), (FWD, 2, 1, 0), (B1, 2, 2, 5), (B0, 2, 2, 1), (IM, 2, 0, 3), (IM, 2, 0, 1),
    (B0, 2, 2, 2), (IM, 2, 0, 2), (B1, 2, 2, 4), (COL, 2, 2, 2), (AC, 2, 0, 0), (B1, 2, 2, 2), (S1, 2, 0, 3),
    (IM, 2, 0, 0), (B1, 2, 2, 3), (B0, 2, 2, 3), (S1, 2, 0, 4), (WORK, 2, 1, 0), (COL, 2, 1, 0), (S1, 2, 1, 0),
    (COL, 2, 1, 1), (S1, 2, 1, 1), (IM, 2, 1, 0), (COL, 2, 1, 2), (B1, 2, 2, 0), (IM, 2, 1, 4), (S1, 2, 1, 2),
    (S1, 2, 1, 3), (B2, 2, 2, 5), (AC, 2, 0, 2), (B1, 2, 2, 1), (IM, 2, 1, 2), (B1, 2, 2, 6), (S1, 2, 1, 4),
    (B2, 2, 2, 2), (AC, 2, 0, 1), (COL, 2, 1, 3), (B2, 2, 2, 3), (IM, 2, 1, 7), (TO, 2, 0, 0), (COL, 2, 0, 3),
    (AC, 2, 1, 0), (AC, 2, 1, 1), (B2, 2, 2, 0), (AC, 2, 0, 4), (S1, 2, 0, 6), (AC, 2, 0, 3), (B2, 2, 2, 4),
    (COL, 2, 2, 3), (AC, 2, 1, 3), (AC, 2, 1, 2), (B3, 2, 2, 5), (IM, 2, 1, 1), (B2, 2, 2, 6), (B3, 2, 2, 2),
    (S1, 2, 0, 5), (B1, 2, 2, 7), (B2, 2, 2, 1), (IM, 2, 0, 5), (B3, 2, 2, 3), (TO, 2, 0, 2), (S1, 2, 0, 7),
    (IM, 2, 0, 7), (TO, 2, 1, 0), (S1, 2, 1, 5), (B3, 2, 2, 4), (TO, 2, 0, 1), (S1, 2, 1, 6), (IM, 2, 0, 6),
    (IM, 2, 1, 3), (B3, 2, 2, 0), (IM, 2, 0, 4), (AC, 2, 0, 6), (TO, 2, 1, 2), (B3, 2, 2, 6), (S1, 2, 1, 7),
    (AC, 2, 1, 4), (B3, 2, 2, 1), (B2, 2, 2, 7), (AC, 2, 0, 5), (IM, 2, 1, 5), (AC, 2, 0, 7), (TO, 2, 1, 1),
    (AC, 2, 1, 5), (AC, 2, 1, 6), (TO, 2, 0, 3), (IM, 2, 1, 6), (BF, 2, 2, 0), (TO, 2, 0, 4), (BI, 2, 2, 1),
    (AC, 2, 1, 7), (BI, 2, 2, 0), (TO, 2, 1, 4), (B3, 2, 2, 7), (TO, 2, 1, 3), (TO, 2, 0, 5), (BA, 2, 2, 1),
    (TO, 2, 0, 6), (TO, 2, 1, 6), (TO, 2, 1, 5), (BA, 2, 2, 0), (BO, 2, 2, 0), (FIN, 2, 0, 0), (FIN, 2, 2, 0),
    (FIN, 2, 1, 0),
)


def bslot(side, level, role):
    return side * 2 + role % 2 if level == 0 else 4 + ((level - 1) * 2 + side) * 4 + role


def scratch(layers):
    bf16, f32, i32, DMA, V = jnp.bfloat16, jnp.float32, jnp.int32, pltpu.SemaphoreType.DMA, pltpu.VMEM
    slabs = (HALF, 4, 128)
    res = dict(
        pack=V(slabs, bf16), inb=V(slabs, bf16), outb=V(slabs, bf16),
        meta=V((16, 128), i32), biasv=V((layers, 4, 1, 128), f32),
        wbuf=V((layers, 4, NZ, NXC, 128, 128), bf16),
        metav=V((4, 8, 128), i32), colv=V((NXC * NZ, 8, 128), i32),
        metas=pltpu.SMEM((4, 8, 128), i32), cols=pltpu.SMEM((NXC * NZ, 8, 128), i32),
        wl_sem=DMA((layers, NZ)), ws_sem=DMA((layers,)), wr_sem=DMA((layers, NZ)),
        ms_sem=DMA((3,)), mr_sem=DMA((3,)), cs_sem=DMA, cr_sem=DMA, loc_sem=DMA((2,)),
        in_s=DMA, in_r=DMA, out_s=DMA, out_r=DMA,
    )
    for i, (kind, m) in enumerate(STREAMS):
        p = (4, m, 128)
        res.update({f"act{i}": V((layers + 1, 4) + p, bf16), f"work{i}": V((4,) + p, bf16),
                    f"ag_s{i}": DMA((layers, 3)), f"ag_r{i}": DMA((layers, 3))})
        if kind == 0:
            res.update({f"yb{i}": V((NZ, 2) + p, bf16), f"yf{i}": V((NZ, 2) + p, f32),
                        f"sx{i}": V((NZ,) + p, bf16), f"sz{i}": V((NZ - 1,) + p, bf16),
                        f"rx{i}": V((layers, 3, NZ) + p, bf16), f"rz{i}": V((layers, NZ - 1) + p, bf16),
                        f"sx_sem{i}": DMA((layers,)), f"rx_sem{i}": DMA((layers, 3, NZ)),
                        f"sz_sem{i}": DMA((layers,)), f"rz_sem{i}": DMA((layers, NZ - 1))})
        else:
            h = (2, m, 128)
            res.update({f"yf{i}": V((NZ, 4) + p, f32),
                        f"sx{i}": V((6,) + h, bf16), f"sz{i}": V((28,) + p, bf16),
                        f"rx{i}": V((layers, 6) + h, bf16), f"rz{i}": V((layers, 28) + p, bf16),
                        f"sx_sem{i}": DMA((layers,)), f"rx_sem{i}": DMA((layers, 6)),
                        f"sz_sem{i}": DMA((layers,)), f"rz_sem{i}": DMA((layers, 28))})
    return res


def layers_kernel(w_hbm, feat, row_in, live_in, col_in, bias, out, *refs):
    f32, bf16 = jnp.float32, jnp.bfloat16
    s = dict(zip(scratch(LAYERS), refs))
    pack, inb, outb, meta, biasv, wbuf = (s[n] for n in ("pack", "inb", "outb", "meta", "biasv", "wbuf"))
    metav, colv, metas, cols = (s[n] for n in ("metav", "colv", "metas", "cols"))
    nx, ny, im = lax.axis_index("nx"), lax.axis_index("ny"), lax.axis_index("img")
    x, c = nx // 2, nx % 2
    yl, z = ny // NZ, ny % NZ
    me = yl * 2 + c
    plane = x * NZ + z
    flat = nx * NY + ny
    layers = LAYERS

    def dev(xx, cc, yy, zz, ii):
        return (xx * 2 + cc, yy * NZ + zz, ii)

    partner = dev(x, 1 - c, yl, z, im)
    near = dev(x, c, 1 - yl, z, im)
    diag = dev(x, 1 - c, 1 - yl, z, im)
    im_up = (im + yl) % 2
    im_dn = (im + 1 - yl) % 2
    x1, x2, x3 = (x + 1) % NXC, (x + 2) % NXC, (x + 3) % NXC
    xp, xm = dev(x1, c, yl, z, im), dev(x3, c, yl, z, im)

    def along_z(hops):
        return dev(x, c, yl, (z + NZ + hops) % NZ, im)

    def plus(k):
        return k % 2 == 1 or k == 0

    def col_z(k):
        far = 4 - (k + 1) // 2
        return (z + NZ + jnp.where(k % 2 == 1, far, -far)) % NZ

    def for_half(fn):
        for b in range(1, NY):
            fn(nx * NY + (ny + b) % NY, (nx, (ny + b) % NY, im))

        def rows(a, carry):
            n = (nx + a) % (2 * NXC)
            for b in range(NY):
                fn(n * NY + (ny + b) % NY, (n, (ny + b) % NY, im))
            return carry

        lax.fori_loop(1, 2 * NXC, rows, 0)

    def for_plane(fn):
        def step(j, carry):
            fn(j, dev((x + j // NZ) % NXC, c, yl, (z + j) % NZ, im))
            return carry

        lax.fori_loop(1, NXC * NZ, step, 0)

    def remote(src, dst, ss, rs, d):
        return pltpu.make_async_remote_copy(src_ref=src, dst_ref=dst, send_sem=ss, recv_sem=rs,
                                            device_id=d, device_id_type=MESH)

    barrier = pltpu.get_barrier_semaphore()

    def greet(k, d):
        pl.semaphore_signal(barrier, inc=1, device_id=d, device_id_type=MESH)

    for cc in (0, 1):
        greet(0, dev(x, cc, 1 - yl, z, 1 - im))
    for_half(greet)
    for r in range(4):
        pack[:, r, :] = feat[:, r, 0, :]
    for i in range(layers):
        meta[i, :] = row_in[i, 0, :]
        meta[3 + i, :] = live_in[i, 0, :]
        meta[8 + i, :] = col_in[i, 0, :]
        for r in range(4):
            biasv[i, r, 0, :] = bias[i, r * 128:(r + 1) * 128]
    metav[me] = meta[pl.ds(0, 8), :]
    colv[plane] = meta[pl.ds(8, 8), :]
    pl.semaphore_wait(barrier, 2 + HALF - 1)

    for_half(lambda k, d: remote(pack.at[k], inb.at[flat], s["in_s"], s["in_r"], d).start())

    def meta_cp(k, d):
        return remote(meta.at[pl.ds(0, 8)], metav.at[me], s["ms_sem"].at[k], s["mr_sem"].at[k], d)

    group = ((0, partner, yl * 2 + 1 - c), (1, near, (1 - yl) * 2 + c), (2, diag, (1 - yl) * 2 + 1 - c))
    for k, d, _ in group:
        meta_cp(k, d).start()
    for_plane(lambda j, d: remote(meta.at[pl.ds(8, 8)], colv.at[plane], s["cs_sem"], s["cr_sem"], d).start())

    def start_weights(l, lo, hi):
        def step(k, carry):
            zz = col_z(k)

            def send(x0, n, cc, yy, ii):
                remote(w_hbm.at[l, pl.ds(x0, n), cc, yy, zz], wbuf.at[l, me, k, pl.ds(x0, n)],
                       s["ws_sem"].at[l], s["wr_sem"].at[l, k], dev(x, cc, yy, z, ii)).start()

            for cc in (0, 1):
                send(0, 2, cc, 1 - yl, im_up)
                send(2, 2, cc, 1 - yl, im_dn)
            send(0, 4, 1 - c, yl, im)
            pltpu.make_async_copy(w_hbm.at[l, :, c, yl, zz], wbuf.at[l, me, k], s["wl_sem"].at[l, k]).start()
            return carry

        lax.fori_loop(lo, hi, step, 0)

    def wait_weights(l, k):
        pltpu.make_async_copy(w_hbm.at[l, :, c, yl, 0], wbuf.at[l, me, k], s["wl_sem"].at[l, k]).wait()
        three = wbuf.at[l, pl.ds(0, 3), k]
        remote(three, three, s["ws_sem"].at[l], s["wr_sem"].at[l, k], partner).wait_recv()

    start_weights(0, 0, FIRST)
    for k, d, src in group:
        remote(meta.at[pl.ds(0, 8)], metav.at[src], s["ms_sem"].at[k], s["mr_sem"].at[k], d).wait_recv()
        meta_cp(k, d).wait_send()
    lot = colv.at[pl.ds(0, NXC * NZ - 1)]
    lot = remote(lot, lot, s["cs_sem"], s["cr_sem"], partner)
    lot.wait_recv()
    lot.wait_send()
    tables = (pltpu.make_async_copy(metav, metas, s["loc_sem"].at[0]),
              pltpu.make_async_copy(colv, cols, s["loc_sem"].at[1]))
    for cp in tables:
        cp.start()
    inb[flat] = pack[flat]
    lot = remote(pack.at[pl.ds(0, HALF - 1)], inb.at[pl.ds(0, HALF - 1)], s["in_s"], s["in_r"], partner)
    lot.wait_recv()
    for r in range(4):
        rows = inb[:, r, :]
        for i, (_, m) in enumerate(STREAMS):
            s[f"act{i}"][0, me, r] = rows[OFFSET[i]:OFFSET[i] + m]

    def ag(l, i, src, slot, d):
        ref = s[f"act{i}"].at[l, src]
        return remote(ref, ref, s[f"ag_s{i}"].at[l, slot], s[f"ag_r{i}"].at[l, slot], d)

    def ags(l, i, _):
        ag(l, i, me, 0, near).start()
        ag(l, i, me, 1, partner).start()

    def fwd(l, i, _):
        ag(l, i, (1 - yl) * 2 + c, 0, near).wait_recv()
        ag(l, i, (1 - yl) * 2 + c, 2, partner).start()

    def sent(l, i):
        for slot in range(3):
            ag(l, i, me, slot, partner).wait_send()
        for a in "xz":
            ref = s[f"r{a}{i}"].at[l]
            remote(ref, ref, s[f"s{a}_sem{i}"].at[l], s["in_r"], partner).wait_send()

    def work(l, i, _):
        ag(l, i, yl * 2 + 1 - c, 1, partner).wait_recv()
        ag(l, i, (1 - yl) * 2 + 1 - c, 2, partner).wait_recv()
        if l > 0:
            sent(l - 1, i)
        for src in range(4):
            s[f"work{i}"][src] = s[f"act{i}"][l, src]

    arrived = set()

    def col(l, i, seg):
        kind, _ = STREAMS[i]
        ks = SEGS[min(l, 1)][seg]
        for k in ks:
            if (l, k) not in arrived:
                arrived.add((l, k))
                wait_weights(l, k)
        held, yf = s[f"work{i}"], s[f"yf{i}"]

        def product(k, xx, zz):
            dest = (xx * 2 + c) * NY + yl * NZ + zz
            parts = [None] * 4
            for src in range(4):
                at = (x * 2 + src % 2) * NY + (src // 2) * NZ + z
                row, live, place = metas[src, l, dest], metas[src, 3 + l, dest], cols[xx * NZ + zz, l, at]
                term = jnp.dot(held[src, row], wbuf[l, src, k, xx], preferred_element_type=f32)
                key = jnp.where(live == 1, place, 4)
                for q in range(4):
                    mine = jnp.where(key == q, term, jnp.zeros_like(term))
                    parts[q] = mine if src == 0 else parts[q] + mine
            return parts

        def step(t, carry):
            k, p = t // 2, t % 2
            zz = col_z(k)
            up = jnp.where(jnp.logical_or(k % 2 == 1, k == 0), 1, 0)
            near_x = jnp.where(up == 1, x1, x3)
            far_x = jnp.where(up == 1, x3, x1)
            one = product(k, jnp.where(p == 0, x2, far_x), zz)
            two = product(k, jnp.where(p == 0, near_x, x), zz)
            for q in range(4):
                a, b = one[q], two[q]
                if kind == 0:
                    s[f"yb{i}"][k, p, q] = a.astype(bf16)
                    yf[k, p, q] = b
                else:
                    yf[k, p * (1 + up), q] = a
                    yf[k, 3 * p + (1 - p) * (2 - up), q] = b
            return carry

        lax.fori_loop(2 * ks[0], 2 * ks[-1] + 2, step, 0)

    def xa(l, i, k, n, src, d):
        return remote(src, s[f"rx{i}"].at[l, n, k], s[f"sx_sem{i}"].at[l], s[f"rx_sem{i}"].at[l, n, k], d)

    def s1(l, i, k):
        xa(l, i, k, 0, s[f"yb{i}"].at[k, 0], xp if plus(k) else xm).start()

    def imm(l, i, k):
        xa(l, i, k, 1, s[f"yb{i}"].at[k, 1], xm if plus(k) else xp).start()

    def acc(l, i, k):
        xa(l, i, k, 0, s[f"sx{i}"].at[k], xp).wait_recv()
        s[f"sx{i}"][k] = (s[f"yf{i}"][k, 0] + s[f"rx{i}"][l, 0, k].astype(f32)).astype(bf16)
        xa(l, i, k, 2, s[f"sx{i}"].at[k], xp if plus(k) else xm).start()

    def za(l, i, k):
        hops = JOIN[k][0]
        return remote(s[f"sz{i}"].at[k], s[f"rz{i}"].at[l, k], s[f"sz_sem{i}"].at[l], s[f"rz_sem{i}"].at[l, k],
                      along_z(hops if plus(k) else -hops))

    def total(l, i, k):
        for n in (1, 2):
            xa(l, i, k, n, s[f"sx{i}"].at[k], xp).wait_recv()
        val = (s[f"yf{i}"][k, 1] + s[f"rx{i}"][l, 1, k].astype(f32)) + s[f"rx{i}"][l, 2, k].astype(f32)
        for j in range(7):
            if JOIN[j][1] == k:
                za(l, i, j).wait_recv()
                val = val + s[f"rz{i}"][l, j].astype(f32)
        if k < 7:
            s[f"sz{i}"][k] = val.astype(bf16)
            za(l, i, k).start()
        else:
            s[f"act{i}"][l + 1, me] = jnp.maximum(val + biasv[l], 0.0).astype(bf16)

    def zb(l, i, side, level, role):
        n = bslot(side, level, role)
        return remote(s[f"sz{i}"].at[n], s[f"rz{i}"].at[l, n], s[f"sz_sem{i}"].at[l], s[f"rz_sem{i}"].at[l, n],
                      along_z(-1 if side else 1))

    def b_step(l, i, level, side, role):
        n = bslot(side, level, role)
        val = s[f"yf{i}"][(UP, DOWN)[side][level], role]
        if level > 1 or (level == 1 and role // 2 == side):
            zb(l, i, side, level - 1, role).wait_recv()
            val = val + s[f"rz{i}"][l, bslot(side, level - 1, role)].astype(f32)
        s[f"sz{i}"][n] = val.astype(bf16)
        zb(l, i, side, level, role).start()

    def xb(l, i, n, d):
        return remote(s[f"sx{i}"].at[n], s[f"rx{i}"].at[l, n], s[f"sx_sem{i}"].at[l], s[f"rx_sem{i}"].at[l, n], d)

    def b_sum(l, i, role):
        val = s[f"yf{i}"][7, role]
        for side in (0, 1):
            zb(l, i, side, 3, role).wait_recv()
            val = val + s[f"rz{i}"][l, bslot(side, 3, role)].astype(f32)
        return val

    def b_far(l, i, _):
        val = b_sum(l, i, 0)
        for n, d in ((0, xp), (1, xm)):
            s[f"sx{i}"][n] = val[2 * n:2 * n + 2].astype(bf16)
            xb(l, i, n, d).start()

    def b_imm(l, i, side):
        val = b_sum(l, i, 1 + side)
        n, hi, lo = 3 + 2 * side, 2 - 2 * side, 2 * side
        s[f"sx{i}"][n] = val[hi:hi + 2].astype(bf16)
        xb(l, i, n, xm if side else xp).start()
        s[f"yf{i}"][7, 1 + side, lo:lo + 2] = val[lo:lo + 2]

    def b_acc(l, i, side):
        n, lo = 2 + 2 * side, 2 * side
        xb(l, i, side, xp).wait_recv()
        s[f"sx{i}"][n] = (s[f"yf{i}"][7, 1 + side, lo:lo + 2] + s[f"rx{i}"][l, side].astype(f32)).astype(bf16)
        xb(l, i, n, xm if side else xp).start()

    def b_own(l, i, _):
        s[f"yf{i}"][7, 3] = b_sum(l, i, 3)

    def fin(l, i, _):
        if STREAMS[i][0] == 0:
            total(l, i, 7)
            return
        for n in range(2, 6):
            xb(l, i, n, xp).wait_recv()
        for lo, a, b in ((0, 2, 5), (2, 3, 4)):
            val = s[f"yf{i}"][7, 3, lo:lo + 2] + s[f"rx{i}"][l, a].astype(f32) + s[f"rx{i}"][l, b].astype(f32)
            s[f"act{i}"][l + 1, me, lo:lo + 2] = jnp.maximum(val + biasv[l, lo:lo + 2], 0.0).astype(bf16)

    steps = {AGS: ags, FWD: fwd, WORK: work, COL: col, S1: s1, IM: imm, AC: acc, TO: total, FIN: fin,
             B0: lambda l, i, r: b_step(l, i, 0, r // 2, r), BF: b_far, BI: b_imm, BA: b_acc, BO: b_own}
    for level, name in ((1, B1), (2, B2), (3, B3)):
        steps[name] = lambda l, i, a, level=level: b_step(l, i, level, a // 4, a % 4)
    count = {}
    tables_held = False
    for name, l, i, arg in ORDER:
        if name == COL and not tables_held:
            tables_held = True
            for cp in tables:
                cp.wait()
        steps[name](l, i, arg)
        if name in (AGS, FWD):
            count[name, l] = count.get((name, l), 0) + 1
            if count[name, l] == len(STREAMS):
                if name == AGS:
                    start_weights(l, EARLY if l else FIRST, NZ)
                elif l < layers - 1:
                    start_weights(l + 1, 0, EARLY)

    for r in range(4):
        for i, (_, m) in enumerate(STREAMS):
            outb[pl.ds(OFFSET[i], m), r, :] = s[f"act{i}"][layers, me, r]
    for_half(lambda k, d: remote(outb.at[k], out.at[flat], s["out_s"], s["out_r"], d).start())
    out[flat] = outb[flat]
    lot.wait_send()
    for i in range(len(STREAMS)):
        sent(layers - 1, i)
    for l in range(layers):
        three = wbuf.at[l, pl.ds(0, 3)]
        remote(three, three, s["ws_sem"].at[l], s["wr_sem"].at[l, 0], partner).wait_send()
    lot = remote(outb.at[pl.ds(0, HALF - 1)], out.at[pl.ds(0, HALF - 1)], s["out_s"], s["out_r"], partner)
    lot.wait_recv()
    lot.wait_send()


def run_layers(w, feat, row, live, col, bias):
    vm = pl.BlockSpec(memory_space=pltpu.VMEM)
    return pl.pallas_call(
        layers_kernel,
        out_shape=jax.ShapeDtypeStruct((HALF, 4, 128), jnp.bfloat16),
        in_specs=[pl.BlockSpec(memory_space=pl.ANY)] + [vm] * 5,
        out_specs=vm,
        scratch_shapes=list(scratch(LAYERS).values()),
        compiler_params=pltpu.CompilerParams(
            collective_id=0, has_side_effects=True, vmem_limit_bytes=60 * 1024 * 1024),
    )(w, feat, row, live, col, bias)


def local(features, link_weight, link_row, link_col, link_live, bias):
    layers = bias.shape[0]
    res = run_layers(link_weight.reshape(layers, NXC, 2, 2, NZ, 128, 128), features.reshape(HALF, 4, 1, 128),
                     link_row, link_live, link_col.transpose(0, 2, 1), bias)
    return res.reshape(features.shape)


def solution(mesh):
    placed = (
        P(("nx", "ny", "img"), None),
        P(None, ("nx", "ny"), None, None, None),
        P(None, ("nx", "ny"), None),
        P(None, None, ("nx", "ny")),
        P(None, ("nx", "ny"), None),
        P(None, ("nx", "ny")),
    )
    return jax.shard_map(
        local, mesh=mesh, in_specs=placed, out_specs=P(("nx", "ny", "img"), None), check_vma=False
    )
```

```python
import jax
import jax.numpy as jnp
from jax import lax
from jax.experimental import pallas as pl
from jax.experimental.pallas import tpu as pltpu
from jax.sharding import PartitionSpec as P

MESH = pl.DeviceIdType.MESH
NXC, NZ = 4, 8
NY = 2 * NZ
HALF = 2 * NXC * NY
LAYERS = 3
STREAMS = ((0, 32), (0, 48), (1, 48))
OFFSET = tuple(sum(m for _, m in STREAMS[:i]) for i in range(len(STREAMS)))
UP = (0, 1, 3, 5)
DOWN = (0, 2, 4, 6)
JOIN = {0: (1, 1), 1: (1, 3), 2: (1, 4), 3: (1, 5), 4: (1, 6), 5: (1, 7), 6: (1, 7)}
FIRST = 2
SPLIT = 5
SEGS = (((0,), (1,), (2,), (3,), (4,), (5,), (6,), (7,)), ((0,), (1, 2), (3, 4), (5, 6, 7)))
AGS, FWD, WORK, COL, S1, IM, AC, TO, FIN, B0, B1, B2, B3, BF, BI, BA, BO = range(17)
ORDER = (
    (AGS, 0, 1, 0), (AGS, 0, 2, 0), (AGS, 0, 0, 0), (FWD, 0, 1, 0), (FWD, 0, 2, 0), (WORK, 0, 1, 0), (COL, 0, 1, 0),
    (S1, 0, 1, 0), (IM, 0, 1, 0), (COL, 0, 1, 1), (S1, 0, 1, 1), (FWD, 0, 0, 0), (WORK, 0, 2, 0), (COL, 0, 2, 0),
    (B0, 0, 2, 0), (B0, 0, 2, 1), (B0, 0, 2, 2), (B0, 0, 2, 3), (IM, 0, 1, 1), (COL, 0, 2, 1), (B1, 0, 2, 3),
    (B1, 0, 2, 2), (WORK, 0, 0, 0), (COL, 0, 0, 0), (S1, 0, 0, 0), (COL, 0, 0, 1), (COL, 0, 1, 2), (COL, 0, 2, 2),
    (AC, 0, 1, 0), (B1, 0, 2, 4), (IM, 0, 1, 2), (S1, 0, 1, 2), (COL, 0, 0, 2), (S1, 0, 0, 2), (S1, 0, 0, 1),
    (IM, 0, 0, 1), (IM, 0, 0, 2), (B1, 0, 2, 5), (IM, 0, 0, 0), (AC, 0, 1, 1), (B1, 0, 2, 0), (B1, 0, 2, 6),
    (COL, 0, 1, 3), (B1, 0, 2, 1), (S1, 0, 1, 3), (COL, 0, 2, 3), (AC, 0, 0, 0), (IM, 0, 1, 3), (B1, 0, 2, 7),
    (COL, 0, 0, 3), (B2, 0, 2, 3), (S1, 0, 0, 3), (IM, 0, 0, 3), (TO, 0, 1, 0), (AC, 0, 1, 2), (B2, 0, 2, 2),
    (AC, 0, 0, 2), (COL, 0, 1, 4), (COL, 0, 2, 4), (S1, 0, 1, 4), (B2, 0, 2, 0), (B2, 0, 2, 4), (IM, 0, 1, 4),
    (COL, 0, 0, 4), (B2, 0, 2, 6), (B2, 0, 2, 5), (S1, 0, 0, 4), (IM, 0, 0, 4), (AC, 0, 0, 1), (B2, 0, 2, 1),
    (B2, 0, 2, 7), (COL, 0, 1, 5), (S1, 0, 1, 5), (COL, 0, 2, 5), (TO, 0, 1, 1), (AC, 0, 1, 3), (B3, 0, 2, 3),
    (IM, 0, 1, 5), (COL, 0, 0, 5), (TO, 0, 1, 2), (TO, 0, 0, 0), (S1, 0, 0, 5), (IM, 0, 0, 5), (TO, 0, 0, 2),
    (B3, 0, 2, 2), (AC, 0, 0, 3), (COL, 0, 2, 6), (COL, 0, 1, 6), (AC, 0, 1, 4), (S1, 0, 1, 6), (COL, 0, 0, 6),
    (B3, 0, 2, 4), (IM, 0, 1, 6), (S1, 0, 0, 6), (B3, 0, 2, 5), (AC, 0, 0, 4), (B3, 0, 2, 6), (B3, 0, 2, 0),
    (B3, 0, 2, 1), (IM, 0, 0, 6), (B3, 0, 2, 7), (AC, 0, 1, 5), (COL, 0, 2, 7), (COL, 0, 1, 7), (S1, 0, 1, 7),
    (COL, 0, 0, 7), (TO, 0, 0, 1), (TO, 0, 1, 3), (S1, 0, 0, 7), (IM, 0, 1, 7), (IM, 0, 0, 7), (AC, 0, 0, 5),
    (TO, 0, 1, 4), (AC, 0, 1, 6), (BF, 0, 2, 0), (AC, 0, 0, 6), (BI, 0, 2, 0), (TO, 0, 0, 4), (BI, 0, 2, 1),
    (TO, 0, 0, 3), (BO, 0, 2, 0), (TO, 0, 1, 5), (AC, 0, 1, 7), (AC, 0, 0, 7), (TO, 0, 1, 6), (BA, 0, 2, 1),
    (BA, 0, 2, 0), (TO, 0, 0, 6), (TO, 0, 0, 5), (FIN, 0, 1, 0), (AGS, 1, 1, 0), (FIN, 0, 2, 0), (AGS, 1, 2, 0),
    (FIN, 0, 0, 0), (AGS, 1, 0, 0), (FWD, 1, 1, 0), (FWD, 1, 2, 0), (WORK, 1, 1, 0), (COL, 1, 1, 0), (S1, 1, 1, 0),
    (IM, 1, 1, 0), (COL, 1, 1, 1), (WORK, 1, 2, 0), (COL, 1, 2, 0), (B0, 1, 2, 0), (FWD, 1, 0, 0), (S1, 1, 1, 2),
    (S1, 1, 1, 1), (COL, 1, 1, 2), (B0, 1, 2, 1), (B0, 1, 2, 2), (IM, 1, 1, 4), (IM, 1, 1, 2), (S1, 1, 1, 3),
    (S1, 1, 1, 4), (B0, 1, 2, 3), (IM, 1, 1, 3), (IM, 1, 1, 1), (COL, 1, 2, 1), (B1, 1, 2, 2), (WORK, 1, 0, 0),
    (COL, 1, 0, 0), (AC, 1, 1, 0), (S1, 1, 0, 0), (B1, 1, 2, 4), (B1, 1, 2, 3), (COL, 1, 0, 1), (S1, 1, 0, 2),
    (S1, 1, 0, 1), (IM, 1, 0, 0), (COL, 1, 2, 2), (B1, 1, 2, 0), (AC, 1, 1, 2), (AC, 1, 1, 1), (B1, 1, 2, 5),
    (COL, 1, 0, 2), (B1, 1, 2, 1), (B1, 1, 2, 6), (S1, 1, 0, 3), (AC, 1, 1, 4), (IM, 1, 0, 2), (S1, 1, 0, 4),
    (IM, 1, 0, 3), (B1, 1, 2, 7), (B2, 1, 2, 2), (IM, 1, 0, 1), (IM, 1, 0, 4), (B2, 1, 2, 4), (B2, 1, 2, 3),
    (AC, 1, 1, 3), (AC, 1, 0, 2), (TO, 1, 1, 0), (B2, 1, 2, 0), (B2, 1, 2, 5), (AC, 1, 0, 0), (B2, 1, 2, 1),
    (TO, 1, 1, 2), (AC, 1, 0, 1), (B2, 1, 2, 6), (COL, 1, 0, 3), (COL, 1, 1, 3), (TO, 1, 1, 1), (S1, 1, 0, 6),
    (S1, 1, 1, 6), (S1, 1, 1, 5), (COL, 1, 2, 3), (TO, 1, 1, 4), (S1, 1, 0, 7), (B3, 1, 2, 4), (AC, 1, 0, 4),
    (B3, 1, 2, 0), (TO, 1, 0, 2), (AC, 1, 0, 3), (S1, 1, 0, 5), (IM, 1, 1, 5), (IM, 1, 1, 6), (S1, 1, 1, 7),
    (IM, 1, 0, 7), (TO, 1, 0, 0), (B2, 1, 2, 7), (B3, 1, 2, 2), (IM, 1, 1, 7), (B3, 1, 2, 3), (IM, 1, 0, 5),
    (B3, 1, 2, 6), (B3, 1, 2, 1), (IM, 1, 0, 6), (B3, 1, 2, 5), (AC, 1, 0, 6), (TO, 1, 1, 3), (AC, 1, 1, 5),
    (AC, 1, 1, 6), (AC, 1, 0, 7), (TO, 1, 0, 1), (BF, 1, 2, 0), (AC, 1, 0, 5), (TO, 1, 0, 4), (B3, 1, 2, 7),
    (AC, 1, 1, 7), (BI, 1, 2, 1), (BI, 1, 2, 0), (TO, 1, 1, 5), (TO, 1, 1, 6), (TO, 1, 0, 6), (TO, 1, 0, 3),
    (BA, 1, 2, 1), (BA, 1, 2, 0), (BO, 1, 2, 0), (FIN, 1, 1, 0), (AGS, 2, 1, 0), (FIN, 1, 2, 0), (AGS, 2, 2, 0),
    (TO, 1, 0, 5), (FWD, 2, 1, 0), (FIN, 1, 0, 0), (AGS, 2, 0, 0), (FWD, 2, 2, 0), (WORK, 2, 1, 0), (COL, 2, 1, 0),
    (S1, 2, 1, 0), (IM, 2, 1, 0), (COL, 2, 1, 1), (S1, 2, 1, 1), (WORK, 2, 2, 0), (COL, 2, 2, 0), (B0, 2, 2, 0),
    (S1, 2, 1, 2), (COL, 2, 1, 2), (FWD, 2, 0, 0), (B0, 2, 2, 2), (B0, 2, 2, 1), (B0, 2, 2, 3), (S1, 2, 1, 3),
    (S1, 2, 1, 4), (IM, 2, 1, 2), (COL, 2, 2, 1), (B1, 2, 2, 2), (B1, 2, 2, 4), (B1, 2, 2, 3), (COL, 2, 2, 2),
    (WORK, 2, 0, 0), (COL, 2, 0, 0), (S1, 2, 0, 0), (AC, 2, 1, 0), (COL, 2, 0, 1), (B1, 2, 2, 0), (AC, 2, 1, 2),
    (S1, 2, 0, 1), (IM, 2, 0, 0), (S1, 2, 0, 2), (AC, 2, 1, 1), (B1, 2, 2, 5), (IM, 2, 0, 1), (COL, 2, 0, 2),
    (B1, 2, 2, 1), (S1, 2, 0, 3), (S1, 2, 0, 4), (IM, 2, 0, 2), (AC, 2, 1, 3), (AC, 2, 1, 4), (B1, 2, 2, 6),
    (B1, 2, 2, 7), (B2, 2, 2, 2), (IM, 2, 0, 3), (IM, 2, 0, 4), (B2, 2, 2, 4), (B2, 2, 2, 3), (IM, 2, 1, 1),
    (AC, 2, 0, 0), (COL, 2, 2, 3), (TO, 2, 1, 0), (B2, 2, 2, 0), (AC, 2, 0, 1), (COL, 2, 1, 3), (B2, 2, 2, 1),
    (AC, 2, 0, 2), (S1, 2, 1, 6), (COL, 2, 0, 3), (S1, 2, 0, 5), (TO, 2, 1, 2), (IM, 2, 1, 3), (IM, 2, 1, 4),
    (S1, 2, 1, 5), (B2, 2, 2, 6), (B2, 2, 2, 5), (AC, 2, 0, 3), (B3, 2, 2, 4), (S1, 2, 0, 6), (IM, 2, 0, 5),
    (B3, 2, 2, 3), (B3, 2, 2, 2), (IM, 2, 0, 6), (IM, 2, 1, 7), (S1, 2, 0, 7), (B2, 2, 2, 7), (IM, 2, 0, 7),
    (IM, 2, 1, 6), (TO, 2, 0, 0), (B3, 2, 2, 0), (TO, 2, 1, 1), (IM, 2, 1, 5), (TO, 2, 0, 2), (S1, 2, 1, 7),
    (B3, 2, 2, 1), (AC, 2, 0, 4), (AC, 2, 0, 5), (AC, 2, 1, 6), (TO, 2, 1, 4), (B3, 2, 2, 6), (AC, 2, 1, 5),
    (AC, 2, 0, 6), (TO, 2, 0, 1), (B3, 2, 2, 5), (BF, 2, 2, 0), (AC, 2, 0, 7), (TO, 2, 1, 3), (B3, 2, 2, 7),
    (AC, 2, 1, 7), (TO, 2, 0, 3), (TO, 2, 0, 4), (BI, 2, 2, 1), (TO, 2, 1, 6), (TO, 2, 1, 5), (BI, 2, 2, 0),
    (BA, 2, 2, 0), (BA, 2, 2, 1), (BO, 2, 2, 0), (TO, 2, 0, 5), (TO, 2, 0, 6), (FIN, 2, 1, 0), (FIN, 2, 2, 0),
    (FIN, 2, 0, 0),
)


def bslot(side, level, role):
    return side * 2 + role % 2 if level == 0 else 4 + ((level - 1) * 2 + side) * 4 + role


def scratch(layers):
    bf16, f32, i32, DMA, V = jnp.bfloat16, jnp.float32, jnp.int32, pltpu.SemaphoreType.DMA, pltpu.VMEM
    slabs = (HALF, 4, 128)
    res = dict(
        pack=V(slabs, bf16), inb=V(slabs, bf16), outb=V(slabs, bf16),
        meta=V((8, 128), i32), cmeta=V((4, 128), i32), biasv=V((layers, 4, 1, 128), f32),
        wbuf=V((layers, 4, NZ, NXC, 128, 128), bf16),
        metav=V((4, 8, 128), i32), colv=V((NXC * NZ, 4, 128), i32),
        metas=pltpu.SMEM((4, 8, 128), i32), cols=pltpu.SMEM((NXC * NZ, 4, 128), i32),
        wl_sem=DMA((layers, NZ)), ws_sem=DMA((layers,)), wr_sem=DMA((layers, NZ)),
        ms_sem=DMA((3,)), mr_sem=DMA((3,)), cs_sem=DMA, cr_sem=DMA, loc_sem=DMA((2,)),
        in_s=DMA, in_r=DMA, out_s=DMA, out_r=DMA,
    )
    for i, (kind, m) in enumerate(STREAMS):
        p = (4, m, 128)
        res.update({f"act{i}": V((layers + 1, 4) + p, bf16), f"work{i}": V((4,) + p, bf16),
                    f"ag_s{i}": DMA((layers, 3)), f"ag_r{i}": DMA((layers, 3))})
        if kind == 0:
            res.update({f"yb{i}": V((NZ, 2) + p, bf16), f"yf{i}": V((NZ, 2) + p, f32),
                        f"sx{i}": V((NZ,) + p, bf16), f"sz{i}": V((NZ - 1,) + p, bf16),
                        f"rx{i}": V((layers, 3, NZ) + p, bf16), f"rz{i}": V((layers, NZ - 1) + p, bf16),
                        f"sx_sem{i}": DMA((layers,)), f"rx_sem{i}": DMA((layers, 3, NZ)),
                        f"sz_sem{i}": DMA((layers,)), f"rz_sem{i}": DMA((layers, NZ - 1))})
        else:
            h = (2, m, 128)
            res.update({f"yf{i}": V((NZ, 4) + p, f32),
                        f"sx{i}": V((6,) + h, bf16), f"sz{i}": V((28,) + p, bf16),
                        f"rx{i}": V((layers, 6) + h, bf16), f"rz{i}": V((layers, 28) + p, bf16),
                        f"sx_sem{i}": DMA((layers,)), f"rx_sem{i}": DMA((layers, 6)),
                        f"sz_sem{i}": DMA((layers,)), f"rz_sem{i}": DMA((layers, 28))})
    return res


def layers_kernel(w_hbm, feat, row_in, live_in, col_in, bias, out, *refs):
    f32, bf16 = jnp.float32, jnp.bfloat16
    s = dict(zip(scratch(LAYERS), refs))
    pack, inb, outb, meta, biasv, wbuf = (s[n] for n in ("pack", "inb", "outb", "meta", "biasv", "wbuf"))
    metav, colv, metas, cols, cmeta = (s[n] for n in ("metav", "colv", "metas", "cols", "cmeta"))
    nx, ny, im = lax.axis_index("nx"), lax.axis_index("ny"), lax.axis_index("img")
    x, c = nx // 2, nx % 2
    yl, z = ny // NZ, ny % NZ
    me = yl * 2 + c
    plane = x * NZ + z
    flat = nx * NY + ny
    layers = LAYERS

    def dev(xx, cc, yy, zz, ii):
        return (xx * 2 + cc, yy * NZ + zz, ii)

    partner = dev(x, 1 - c, yl, z, im)
    near = dev(x, c, 1 - yl, z, im)
    diag = dev(x, 1 - c, 1 - yl, z, im)
    im_up = (im + yl) % 2
    im_dn = (im + 1 - yl) % 2
    x1, x2, x3 = (x + 1) % NXC, (x + 2) % NXC, (x + 3) % NXC
    xp, xm = dev(x1, c, yl, z, im), dev(x3, c, yl, z, im)

    def along_z(hops):
        return dev(x, c, yl, (z + NZ + hops) % NZ, im)

    def plus(k):
        return k % 2 == 1 or k == 0

    def col_z(k):
        far = 4 - (k + 1) // 2
        return (z + NZ + jnp.where(k % 2 == 1, far, -far)) % NZ

    spread = (4, 12, 3, 13, 5, 11, 2, 14, 6, 10, 1, 15, 7, 9, 8)

    def for_half(fn):
        def rows(t, carry):
            n = (nx + 4 + (t + 1) // 2 * (1 - 2 * (t % 2))) % (2 * NXC)
            for b in spread + (0,):
                fn(n * NY + (ny + b) % NY, (n, (ny + b) % NY, im))
            return carry

        lax.fori_loop(0, 2 * NXC - 1, rows, 0)
        for b in spread:
            fn(nx * NY + (ny + b) % NY, (nx, (ny + b) % NY, im))

    def for_plane(fn):
        def step(j, carry):
            fn(j, dev((x + j // NZ) % NXC, c, yl, (z + j) % NZ, im))
            return carry

        lax.fori_loop(1, NXC * NZ, step, 0)

    def remote(src, dst, ss, rs, d):
        return pltpu.make_async_remote_copy(src_ref=src, dst_ref=dst, send_sem=ss, recv_sem=rs,
                                            device_id=d, device_id_type=MESH)

    barrier = pltpu.get_barrier_semaphore()

    def greet(k, d):
        pl.semaphore_signal(barrier, inc=1, device_id=d, device_id_type=MESH)

    for cc in (0, 1):
        greet(0, dev(x, cc, 1 - yl, z, 1 - im))
    for_half(greet)
    for r in range(4):
        pack[:, r, :] = feat[:, r, 0, :]
    for i in range(layers):
        meta[i, :] = row_in[i, 0, :]
        meta[3 + i, :] = live_in[i, 0, :]
        cmeta[i, :] = col_in[i, 0, :]
        for r in range(4):
            biasv[i, r, 0, :] = bias[i, r * 128:(r + 1) * 128]
    cmeta[3, :] = cmeta[0, :]
    meta[6, :] = meta[0, :]
    meta[7, :] = meta[0, :]
    metav[me] = meta[...]
    colv[plane] = cmeta[...]
    pl.semaphore_wait(barrier, 2 + HALF - 1)

    for_half(lambda k, d: remote(pack.at[k], inb.at[flat], s["in_s"], s["in_r"], d).start())

    def meta_cp(k, d):
        return remote(meta, metav.at[me], s["ms_sem"].at[k], s["mr_sem"].at[k], d)

    group = ((0, partner, yl * 2 + 1 - c), (1, near, (1 - yl) * 2 + c), (2, diag, (1 - yl) * 2 + 1 - c))
    for k, d, _ in group:
        meta_cp(k, d).start()

    def start_weights(l, lo, hi):
        def column_copies(k, both):
            zz = col_z(k)

            def send(x0, n, cc, yy, ii):
                remote(w_hbm.at[l, pl.ds(x0, n), cc, yy, zz], wbuf.at[l, me, k, pl.ds(x0, n)],
                       s["ws_sem"].at[l], s["wr_sem"].at[l, k], dev(x, cc, yy, z, ii)).start()

            for cc in (0, 1):
                if both:
                    send(0, 2, cc, 1 - yl, im_up)
                    send(2, 2, cc, 1 - yl, im_dn)
                else:
                    send(0, 4, cc, 1 - yl, 1 - im)
            send(0, 4, 1 - c, yl, im)
            pltpu.make_async_copy(w_hbm.at[l, :, c, yl, zz], wbuf.at[l, me, k], s["wl_sem"].at[l, k]).start()

        def step(both):
            def run(k, carry):
                column_copies(k, both)
                return carry

            return run

        split = SPLIT if l else NZ
        if lo < split:
            lax.fori_loop(lo, min(hi, split), step(True), 0)
        if hi > split:
            lax.fori_loop(max(lo, split), hi, step(False), 0)

    def wait_weights(l, k):
        pltpu.make_async_copy(w_hbm.at[l, :, c, yl, 0], wbuf.at[l, me, k], s["wl_sem"].at[l, k]).wait()
        three = wbuf.at[l, pl.ds(0, 3), k]
        remote(three, three, s["ws_sem"].at[l], s["wr_sem"].at[l, k], partner).wait_recv()

    start_weights(0, 0, FIRST)
    for_plane(lambda j, d: remote(cmeta, colv.at[plane], s["cs_sem"], s["cr_sem"], d).start())
    inb[flat] = pack[flat]
    lot = remote(pack.at[pl.ds(0, HALF - 1)], inb.at[pl.ds(0, HALF - 1)], s["in_s"], s["in_r"], partner)
    lot.wait_recv()
    for r in range(4):
        rows = inb[:, r, :]
        for i, (_, m) in enumerate(STREAMS):
            s[f"act{i}"][0, me, r] = rows[OFFSET[i]:OFFSET[i] + m]

    tables = (pltpu.make_async_copy(metav, metas, s["loc_sem"].at[0]),
              pltpu.make_async_copy(colv, cols, s["loc_sem"].at[1]))

    def take_tables():
        for k, d, src in group:
            remote(meta, metav.at[src], s["ms_sem"].at[k], s["mr_sem"].at[k], d).wait_recv()
            meta_cp(k, d).wait_send()
        most = colv.at[pl.ds(0, NXC * NZ - 1)]
        most = remote(most, most, s["cs_sem"], s["cr_sem"], partner)
        most.wait_recv()
        most.wait_send()
        for cp in tables:
            cp.start()

    def ag(l, i, src, slot, d):
        ref = s[f"act{i}"].at[l, src]
        return remote(ref, ref, s[f"ag_s{i}"].at[l, slot], s[f"ag_r{i}"].at[l, slot], d)

    def ags(l, i, _):
        ag(l, i, me, 0, near).start()
        ag(l, i, me, 1, partner).start()

    def fwd(l, i, _):
        ag(l, i, (1 - yl) * 2 + c, 0, near).wait_recv()
        ag(l, i, (1 - yl) * 2 + c, 2, partner).start()

    def sent(l, i):
        for slot in range(3):
            ag(l, i, me, slot, partner).wait_send()
        for a in "xz":
            ref = s[f"r{a}{i}"].at[l]
            remote(ref, ref, s[f"s{a}_sem{i}"].at[l], s["in_r"], partner).wait_send()

    def work(l, i, _):
        ag(l, i, yl * 2 + 1 - c, 1, partner).wait_recv()
        ag(l, i, (1 - yl) * 2 + 1 - c, 2, partner).wait_recv()
        if l > 0:
            sent(l - 1, i)
        for src in range(4):
            s[f"work{i}"][src] = s[f"act{i}"][l, src]

    arrived = set()

    def col(l, i, seg):
        kind, _ = STREAMS[i]
        ks = SEGS[min(l, 1)][seg]
        for k in ks:
            if (l, k) not in arrived:
                arrived.add((l, k))
                wait_weights(l, k)
        held, yf = s[f"work{i}"], s[f"yf{i}"]

        def product(k, xx, zz):
            dest = (xx * 2 + c) * NY + yl * NZ + zz
            parts = [None] * 4
            for src in range(4):
                at = (x * 2 + src % 2) * NY + (src // 2) * NZ + z
                row, live, place = metas[src, l, dest], metas[src, 3 + l, dest], cols[xx * NZ + zz, l, at]
                term = jnp.dot(held[src, row], wbuf[l, src, k, xx], preferred_element_type=f32)
                key = jnp.where(live == 1, place, 4)
                for q in range(4):
                    mine = jnp.where(key == q, term, jnp.zeros_like(term))
                    parts[q] = mine if src == 0 else parts[q] + mine
            return parts

        def step(t, carry):
            k, p = t // 2, t % 2
            zz = col_z(k)
            up = jnp.where(jnp.logical_or(k % 2 == 1, k == 0), 1, 0)
            near_x = jnp.where(up == 1, x1, x3)
            far_x = jnp.where(up == 1, x3, x1)
            one = product(k, jnp.where(p == 0, x2, far_x), zz)
            two = product(k, jnp.where(p == 0, near_x, x), zz)
            for q in range(4):
                a, b = one[q], two[q]
                if kind == 0:
                    s[f"yb{i}"][k, p, q] = a.astype(bf16)
                    yf[k, p, q] = b
                else:
                    yf[k, p * (1 + up), q] = a
                    yf[k, 3 * p + (1 - p) * (2 - up), q] = b
            return carry

        lax.fori_loop(2 * ks[0], 2 * ks[-1] + 2, step, 0)

    def xa(l, i, k, n, src, d):
        return remote(src, s[f"rx{i}"].at[l, n, k], s[f"sx_sem{i}"].at[l], s[f"rx_sem{i}"].at[l, n, k], d)

    def s1(l, i, k):
        xa(l, i, k, 0, s[f"yb{i}"].at[k, 0], xp if plus(k) else xm).start()

    def imm(l, i, k):
        xa(l, i, k, 1, s[f"yb{i}"].at[k, 1], xm if plus(k) else xp).start()

    def acc(l, i, k):
        xa(l, i, k, 0, s[f"sx{i}"].at[k], xp).wait_recv()
        s[f"sx{i}"][k] = (s[f"yf{i}"][k, 0] + s[f"rx{i}"][l, 0, k].astype(f32)).astype(bf16)
        xa(l, i, k, 2, s[f"sx{i}"].at[k], xp if plus(k) else xm).start()

    def za(l, i, k):
        hops = JOIN[k][0]
        return remote(s[f"sz{i}"].at[k], s[f"rz{i}"].at[l, k], s[f"sz_sem{i}"].at[l], s[f"rz_sem{i}"].at[l, k],
                      along_z(hops if plus(k) else -hops))

    def total(l, i, k):
        for n in (1, 2):
            xa(l, i, k, n, s[f"sx{i}"].at[k], xp).wait_recv()
        val = (s[f"yf{i}"][k, 1] + s[f"rx{i}"][l, 1, k].astype(f32)) + s[f"rx{i}"][l, 2, k].astype(f32)
        for j in range(7):
            if JOIN[j][1] == k:
                za(l, i, j).wait_recv()
                val = val + s[f"rz{i}"][l, j].astype(f32)
        if k < 7:
            s[f"sz{i}"][k] = val.astype(bf16)
            za(l, i, k).start()
        else:
            s[f"act{i}"][l + 1, me] = jnp.maximum(val + biasv[l], 0.0).astype(bf16)

    def zb(l, i, side, level, role):
        n = bslot(side, level, role)
        return remote(s[f"sz{i}"].at[n], s[f"rz{i}"].at[l, n], s[f"sz_sem{i}"].at[l], s[f"rz_sem{i}"].at[l, n],
                      along_z(-1 if side else 1))

    def b_step(l, i, level, side, role):
        n = bslot(side, level, role)
        val = s[f"yf{i}"][(UP, DOWN)[side][level], role]
        if level > 1 or (level == 1 and role // 2 == side):
            zb(l, i, side, level - 1, role).wait_recv()
            val = val + s[f"rz{i}"][l, bslot(side, level - 1, role)].astype(f32)
        s[f"sz{i}"][n] = val.astype(bf16)
        zb(l, i, side, level, role).start()

    def xb(l, i, n, d):
        return remote(s[f"sx{i}"].at[n], s[f"rx{i}"].at[l, n], s[f"sx_sem{i}"].at[l], s[f"rx_sem{i}"].at[l, n], d)

    def b_sum(l, i, role):
        val = s[f"yf{i}"][7, role]
        for side in (0, 1):
            zb(l, i, side, 3, role).wait_recv()
            val = val + s[f"rz{i}"][l, bslot(side, 3, role)].astype(f32)
        return val

    def b_far(l, i, _):
        val = b_sum(l, i, 0)
        for n, d in ((0, xp), (1, xm)):
            s[f"sx{i}"][n] = val[2 * n:2 * n + 2].astype(bf16)
            xb(l, i, n, d).start()

    def b_imm(l, i, side):
        val = b_sum(l, i, 1 + side)
        n, hi, lo = 3 + 2 * side, 2 - 2 * side, 2 * side
        s[f"sx{i}"][n] = val[hi:hi + 2].astype(bf16)
        xb(l, i, n, xm if side else xp).start()
        s[f"yf{i}"][7, 1 + side, lo:lo + 2] = val[lo:lo + 2]

    def b_acc(l, i, side):
        n, lo = 2 + 2 * side, 2 * side
        xb(l, i, side, xp).wait_recv()
        s[f"sx{i}"][n] = (s[f"yf{i}"][7, 1 + side, lo:lo + 2] + s[f"rx{i}"][l, side].astype(f32)).astype(bf16)
        xb(l, i, n, xm if side else xp).start()

    def b_own(l, i, _):
        s[f"yf{i}"][7, 3] = b_sum(l, i, 3)

    def fin(l, i, _):
        if STREAMS[i][0] == 0:
            total(l, i, 7)
            return
        for n in range(2, 6):
            xb(l, i, n, xp).wait_recv()
        for lo, a, b in ((0, 2, 5), (2, 3, 4)):
            val = s[f"yf{i}"][7, 3, lo:lo + 2] + s[f"rx{i}"][l, a].astype(f32) + s[f"rx{i}"][l, b].astype(f32)
            s[f"act{i}"][l + 1, me, lo:lo + 2] = jnp.maximum(val + biasv[l, lo:lo + 2], 0.0).astype(bf16)

    steps = {AGS: ags, FWD: fwd, WORK: work, COL: col, S1: s1, IM: imm, AC: acc, TO: total, FIN: fin,
             B0: lambda l, i, r: b_step(l, i, 0, r // 2, r), BF: b_far, BI: b_imm, BA: b_acc, BO: b_own}
    for level, name in ((1, B1), (2, B2), (3, B3)):
        steps[name] = lambda l, i, a, level=level: b_step(l, i, level, a // 4, a % 4)
    count = {}
    tables_held = False
    for name, l, i, arg in ORDER:
        if name == COL and not tables_held:
            tables_held = True
            for cp in tables:
                cp.wait()
        steps[name](l, i, arg)
        if name == AGS and l == 0 or name == FWD:
            count[name, l] = count.get((name, l), 0) + 1
            if count[name, l] == len(STREAMS):
                if name == AGS:
                    start_weights(0, FIRST, NZ)
                    take_tables()
                elif l < layers - 1:
                    start_weights(l + 1, 0, NZ)

    for r in range(4):
        for i, (_, m) in enumerate(STREAMS):
            outb[pl.ds(OFFSET[i], m), r, :] = s[f"act{i}"][layers, me, r]
    for_half(lambda k, d: remote(outb.at[k], out.at[flat], s["out_s"], s["out_r"], d).start())
    out[flat] = outb[flat]
    lot.wait_send()
    for i in range(len(STREAMS)):
        sent(layers - 1, i)
    for l in range(layers):
        three = wbuf.at[l, pl.ds(0, 3)]
        remote(three, three, s["ws_sem"].at[l], s["wr_sem"].at[l, 0], partner).wait_send()
    lot = remote(outb.at[pl.ds(0, HALF - 1)], out.at[pl.ds(0, HALF - 1)], s["out_s"], s["out_r"], partner)
    lot.wait_recv()
    lot.wait_send()


def run_layers(w, feat, row, live, col, bias):
    vm = pl.BlockSpec(memory_space=pltpu.VMEM)
    return pl.pallas_call(
        layers_kernel,
        out_shape=jax.ShapeDtypeStruct((HALF, 4, 128), jnp.bfloat16),
        in_specs=[pl.BlockSpec(memory_space=pl.ANY)] + [vm] * 5,
        out_specs=vm,
        scratch_shapes=list(scratch(LAYERS).values()),
        compiler_params=pltpu.CompilerParams(
            collective_id=0, has_side_effects=True, vmem_limit_bytes=60 * 1024 * 1024),
    )(w, feat, row, live, col, bias)


def local(features, link_weight, link_row, link_col, link_live, bias):
    layers = bias.shape[0]
    res = run_layers(link_weight.reshape(layers, NXC, 2, 2, NZ, 128, 128), features.reshape(HALF, 4, 1, 128),
                     link_row, link_live, link_col.transpose(0, 2, 1), bias)
    return res.reshape(features.shape)


def solution(mesh):
    placed = (
        P(("nx", "ny", "img"), None),
        P(None, ("nx", "ny"), None, None, None),
        P(None, ("nx", "ny"), None),
        P(None, None, ("nx", "ny")),
        P(None, ("nx", "ny"), None),
        P(None, ("nx", "ny")),
    )
    return jax.shard_map(
        local, mesh=mesh, in_specs=placed, out_specs=P(("nx", "ny", "img"), None), check_vma=False
    )
```

```python
import jax
import jax.numpy as jnp
from jax import lax
from jax.experimental import pallas as pl
from jax.experimental.pallas import tpu as pltpu
from jax.sharding import PartitionSpec as P

MESH = pl.DeviceIdType.MESH
NXC, NZ = 4, 8
NY = 2 * NZ
HALF = 2 * NXC * NY
LAYERS = 3
STREAMS = ((0, 32), (0, 48), (1, 48))
OFFSET = tuple(sum(m for _, m in STREAMS[:i]) for i in range(len(STREAMS)))
UP = (0, 1, 3, 5)
DOWN = (0, 2, 4, 6)
JOIN = {0: (1, 1), 1: (1, 3), 2: (1, 4), 3: (1, 5), 4: (1, 6), 5: (1, 7), 6: (1, 7)}
FIRST = 2
SPLIT = 5
SEGS = (((0,), (1,), (2,), (3,), (4,), (5,), (6,), (7,)), ((0,), (1, 2), (3, 4), (5, 6, 7)))
AGS, FWD, WORK, COL, S1, IM, AC, TO, FIN, B0, B1, B2, B3, BF, BI, BA, BO = range(17)
ORDER = (
    (AGS, 0, 2, 0), (AGS, 0, 1, 0), (AGS, 0, 0, 0), (FWD, 0, 2, 0), (FWD, 0, 1, 0), (WORK, 0, 2, 0), (COL, 0, 2, 0),
    (B0, 0, 2, 0), (COL, 0, 2, 1), (B1, 0, 2, 3), (B1, 0, 2, 2), (FWD, 0, 0, 0), (B0, 0, 2, 2), (B0, 0, 2, 1),
    (WORK, 0, 1, 0), (B0, 0, 2, 3), (COL, 0, 1, 0), (IM, 0, 1, 0), (S1, 0, 1, 0), (COL, 0, 1, 1), (S1, 0, 1, 1),
    (IM, 0, 1, 1), (WORK, 0, 0, 0), (COL, 0, 0, 0), (IM, 0, 0, 0), (S1, 0, 0, 0), (COL, 0, 0, 1), (IM, 0, 0, 1),
    (COL, 0, 0, 2), (S1, 0, 0, 2), (S1, 0, 0, 1), (COL, 0, 2, 2), (B1, 0, 2, 5), (IM, 0, 0, 2), (B1, 0, 2, 4),
    (COL, 0, 1, 2), (B1, 0, 2, 6), (IM, 0, 1, 2), (S1, 0, 1, 2), (B1, 0, 2, 0), (AC, 0, 1, 0), (B1, 0, 2, 7),
    (COL, 0, 2, 3), (AC, 0, 1, 1), (COL, 0, 0, 3), (S1, 0, 0, 3), (IM, 0, 0, 3), (B2, 0, 2, 2), (COL, 0, 1, 3),
    (B1, 0, 2, 1), (IM, 0, 1, 3), (S1, 0, 1, 3), (AC, 0, 0, 0), (B2, 0, 2, 3), (AC, 0, 0, 1), (AC, 0, 0, 2),
    (B2, 0, 2, 0), (COL, 0, 1, 4), (COL, 0, 2, 4), (B2, 0, 2, 5), (AC, 0, 1, 2), (IM, 0, 1, 4), (S1, 0, 1, 4),
    (B2, 0, 2, 4), (COL, 0, 0, 4), (B2, 0, 2, 6), (S1, 0, 0, 4), (IM, 0, 0, 4), (TO, 0, 1, 0), (B2, 0, 2, 7),
    (COL, 0, 0, 5), (COL, 0, 2, 5), (S1, 0, 0, 5), (B2, 0, 2, 1), (IM, 0, 0, 5), (B3, 0, 2, 2), (TO, 0, 0, 2),
    (COL, 0, 1, 5), (S1, 0, 1, 5), (B3, 0, 2, 3), (AC, 0, 0, 3), (IM, 0, 1, 5), (AC, 0, 1, 3), (TO, 0, 1, 2),
    (B3, 0, 2, 0), (TO, 0, 0, 0), (COL, 0, 1, 6), (S1, 0, 1, 6), (COL, 0, 2, 6), (AC, 0, 1, 4), (B3, 0, 2, 4),
    (AC, 0, 0, 4), (B3, 0, 2, 5), (B3, 0, 2, 6), (IM, 0, 1, 6), (COL, 0, 0, 6), (IM, 0, 0, 6), (S1, 0, 0, 6),
    (TO, 0, 1, 1), (B3, 0, 2, 1), (B3, 0, 2, 7), (AC, 0, 0, 5), (COL, 0, 0, 7), (IM, 0, 0, 7), (COL, 0, 1, 7),
    (AC, 0, 1, 5), (IM, 0, 1, 7), (COL, 0, 2, 7), (AC, 0, 1, 6), (S1, 0, 1, 7), (S1, 0, 0, 7), (BF, 0, 2, 0),
    (TO, 0, 1, 4), (TO, 0, 0, 1), (TO, 0, 0, 4), (AC, 0, 0, 6), (TO, 0, 1, 3), (BI, 0, 2, 1), (BI, 0, 2, 0),
    (BO, 0, 2, 0), (TO, 0, 0, 3), (TO, 0, 1, 6), (BA, 0, 2, 1), (AC, 0, 1, 7), (TO, 0, 1, 5), (TO, 0, 0, 6),
    (AC, 0, 0, 7), (BA, 0, 2, 0), (TO, 0, 0, 5), (FIN, 0, 1, 0), (AGS, 1, 1, 0), (FIN, 0, 2, 0), (AGS, 1, 2, 0),
    (FIN, 0, 0, 0), (AGS, 1, 0, 0), (FWD, 1, 1, 0), (FWD, 1, 2, 0), (WORK, 1, 1, 0), (COL, 1, 1, 0), (IM, 1, 1, 0),
    (S1, 1, 1, 0), (FWD, 1, 0, 0), (COL, 1, 1, 1), (S1, 1, 1, 2), (S1, 1, 1, 1), (WORK, 1, 2, 0), (COL, 1, 2, 0),
    (B0, 1, 2, 0), (B0, 1, 2, 2), (B0, 1, 2, 3), (WORK, 1, 0, 0), (COL, 1, 0, 0), (S1, 1, 0, 0), (IM, 1, 0, 0),
    (COL, 1, 0, 1), (S1, 1, 0, 2), (IM, 1, 0, 2), (COL, 1, 0, 2), (AC, 1, 1, 0), (S1, 1, 0, 4), (S1, 1, 0, 3),
    (IM, 1, 0, 3), (IM, 1, 0, 1), (B0, 1, 2, 1), (COL, 1, 2, 1), (B1, 1, 2, 2), (AC, 1, 1, 1), (AC, 1, 1, 2),
    (B1, 1, 2, 3), (B1, 1, 2, 4), (S1, 1, 0, 1), (IM, 1, 1, 1), (B1, 1, 2, 5), (IM, 1, 1, 2), (COL, 1, 2, 2),
    (B1, 1, 2, 0), (B1, 1, 2, 6), (AC, 1, 0, 0), (IM, 1, 0, 4), (COL, 1, 1, 2), (S1, 1, 1, 3), (B1, 1, 2, 7),
    (S1, 1, 1, 4), (IM, 1, 1, 4), (IM, 1, 1, 3), (AC, 1, 0, 2), (AC, 1, 0, 4), (TO, 1, 1, 0), (B1, 1, 2, 1),
    (AC, 1, 0, 3), (B2, 1, 2, 2), (B2, 1, 2, 4), (B2, 1, 2, 3), (B2, 1, 2, 5), (AC, 1, 0, 1), (B2, 1, 2, 0),
    (B2, 1, 2, 6), (TO, 1, 1, 2), (COL, 1, 0, 3), (AC, 1, 1, 4), (IM, 1, 0, 5), (B2, 1, 2, 7), (S1, 1, 0, 5),
    (TO, 1, 1, 1), (TO, 1, 0, 0), (IM, 1, 0, 6), (IM, 1, 0, 7), (COL, 1, 2, 3), (B3, 1, 2, 4), (AC, 1, 1, 3),
    (B3, 1, 2, 2), (B2, 1, 2, 1), (TO, 1, 0, 2), (S1, 1, 0, 6), (COL, 1, 1, 3), (S1, 1, 1, 6), (S1, 1, 1, 5),
    (B3, 1, 2, 3), (IM, 1, 1, 7), (S1, 1, 1, 7), (B3, 1, 2, 6), (IM, 1, 1, 6), (B3, 1, 2, 5), (IM, 1, 1, 5),
    (S1, 1, 0, 7), (B3, 1, 2, 0), (TO, 1, 1, 4), (AC, 1, 0, 5), (B3, 1, 2, 7), (TO, 1, 0, 1), (TO, 1, 1, 3),
    (AC, 1, 0, 6), (TO, 1, 0, 4), (AC, 1, 1, 5), (AC, 1, 1, 6), (B3, 1, 2, 1), (BI, 1, 2, 1), (AC, 1, 1, 7),
    (BF, 1, 2, 0), (AC, 1, 0, 7), (TO, 1, 0, 3), (BO, 1, 2, 0), (TO, 1, 1, 6), (TO, 1, 0, 6), (TO, 1, 1, 5),
    (BI, 1, 2, 0), (BA, 1, 2, 1), (BA, 1, 2, 0), (TO, 1, 0, 5), (FIN, 1, 1, 0), (AGS, 2, 1, 0), (FIN, 1, 2, 0),
    (AGS, 2, 2, 0), (FIN, 1, 0, 0), (AGS, 2, 0, 0), (FWD, 2, 1, 0), (FWD, 2, 2, 0), (WORK, 2, 1, 0), (COL, 2, 1, 0),
    (IM, 2, 1, 0), (FWD, 2, 0, 0), (S1, 2, 1, 0), (COL, 2, 1, 1), (WORK, 2, 2, 0), (S1, 2, 1, 1), (IM, 2, 1, 1),
    (COL, 2, 2, 0), (B0, 2, 2, 0), (B0, 2, 2, 1), (WORK, 2, 0, 0), (COL, 2, 0, 0), (IM, 2, 0, 0), (S1, 2, 0, 0),
    (S1, 2, 1, 2), (B0, 2, 2, 3), (IM, 2, 1, 2), (B0, 2, 2, 2), (COL, 2, 0, 1), (S1, 2, 0, 2), (S1, 2, 0, 1),
    (COL, 2, 2, 1), (B1, 2, 2, 3), (B1, 2, 2, 2), (B1, 2, 2, 4), (B1, 2, 2, 5), (AC, 2, 1, 0), (COL, 2, 0, 2),
    (S1, 2, 0, 4), (S1, 2, 0, 3), (IM, 2, 0, 3), (COL, 2, 2, 2), (B1, 2, 2, 0), (B1, 2, 2, 7), (AC, 2, 0, 0),
    (COL, 2, 1, 2), (IM, 2, 1, 4), (B1, 2, 2, 6), (S1, 2, 1, 3), (AC, 2, 1, 2), (S1, 2, 1, 4), (B1, 2, 2, 1),
    (IM, 2, 1, 3), (IM, 2, 0, 1), (AC, 2, 1, 1), (AC, 2, 0, 1), (IM, 2, 0, 2), (AC, 2, 0, 2), (IM, 2, 0, 4),
    (B2, 2, 2, 3), (B2, 2, 2, 4), (TO, 2, 1, 0), (AC, 2, 0, 4), (B2, 2, 2, 2), (AC, 2, 0, 3), (B2, 2, 2, 5),
    (COL, 2, 0, 3), (IM, 2, 0, 6), (S1, 2, 0, 5), (IM, 2, 0, 7), (TO, 2, 0, 0), (B2, 2, 2, 7), (COL, 2, 2, 3),
    (B3, 2, 2, 3), (AC, 2, 1, 4), (B2, 2, 2, 6), (S1, 2, 0, 6), (B2, 2, 2, 0), (B3, 2, 2, 4), (AC, 2, 1, 3),
    (B2, 2, 2, 1), (COL, 2, 1, 3), (S1, 2, 1, 6), (S1, 2, 1, 5), (IM, 2, 1, 7), (B3, 2, 2, 5), (IM, 2, 1, 5),
    (IM, 2, 1, 6), (TO, 2, 1, 2), (S1, 2, 0, 7), (TO, 2, 1, 1), (IM, 2, 0, 5), (B3, 2, 2, 2), (S1, 2, 1, 7),
    (TO, 2, 0, 2), (B3, 2, 2, 7), (TO, 2, 0, 1), (B3, 2, 2, 6), (B3, 2, 2, 0), (AC, 2, 0, 5), (AC, 2, 0, 6),
    (B3, 2, 2, 1), (AC, 2, 1, 6), (TO, 2, 1, 3), (TO, 2, 1, 4), (AC, 2, 1, 5), (TO, 2, 0, 4), (TO, 2, 0, 3),
    (BO, 2, 2, 0), (AC, 2, 0, 7), (BF, 2, 2, 0), (BI, 2, 2, 1), (AC, 2, 1, 7), (BI, 2, 2, 0), (TO, 2, 1, 6),
    (TO, 2, 0, 6), (TO, 2, 1, 5), (TO, 2, 0, 5), (BA, 2, 2, 0), (BA, 2, 2, 1), (FIN, 2, 1, 0), (FIN, 2, 2, 0),
    (FIN, 2, 0, 0),
)


def bslot(side, level, role):
    return side * 2 + role % 2 if level == 0 else 4 + ((level - 1) * 2 + side) * 4 + role


def scratch(layers):
    bf16, f32, i32, DMA, V = jnp.bfloat16, jnp.float32, jnp.int32, pltpu.SemaphoreType.DMA, pltpu.VMEM
    slabs = (HALF, 4, 128)
    res = dict(
        pack=V(slabs, bf16), inb=V(slabs, bf16), outb=V(slabs, bf16),
        meta=V((8, 128), i32), cmeta=V((4, 128), i32), biasv=V((layers, 4, 1, 128), f32),
        wbuf=V((layers, 4, NZ, NXC, 128, 128), bf16),
        metav=V((4, 8, 128), i32), colv=V((NXC * NZ, 4, 128), i32),
        metas=pltpu.SMEM((4, 8, 128), i32), cols=pltpu.SMEM((NXC * NZ, 4, 128), i32),
        wl_sem=DMA((layers, NZ)), ws_sem=DMA((layers,)), wr_sem=DMA((layers, NZ)),
        ms_sem=DMA((3,)), mr_sem=DMA((3,)), cs_sem=DMA, cr_sem=DMA, loc_sem=DMA((2,)),
        in_s=DMA, in_r=DMA, out_s=DMA, out_r=DMA,
    )
    for i, (kind, m) in enumerate(STREAMS):
        p = (4, m, 128)
        res.update({f"act{i}": V((layers + 1, 4) + p, bf16), f"work{i}": V((4,) + p, bf16),
                    f"ag_s{i}": DMA((layers, 3)), f"ag_r{i}": DMA((layers, 3))})
        if kind == 0:
            res.update({f"yb{i}": V((NZ, 2) + p, bf16), f"yf{i}": V((NZ, 2) + p, f32),
                        f"sx{i}": V((NZ,) + p, bf16), f"sz{i}": V((NZ - 1,) + p, bf16),
                        f"rx{i}": V((layers, 3, NZ) + p, bf16), f"rz{i}": V((layers, NZ - 1) + p, bf16),
                        f"sx_sem{i}": DMA((layers,)), f"rx_sem{i}": DMA((layers, 3, NZ)),
                        f"sz_sem{i}": DMA((layers,)), f"rz_sem{i}": DMA((layers, NZ - 1))})
        else:
            h = (2, m, 128)
            res.update({f"yf{i}": V((NZ, 4) + p, f32),
                        f"sx{i}": V((6,) + h, bf16), f"sz{i}": V((28,) + p, bf16),
                        f"rx{i}": V((layers, 6) + h, bf16), f"rz{i}": V((layers, 28) + p, bf16),
                        f"sx_sem{i}": DMA((layers,)), f"rx_sem{i}": DMA((layers, 6)),
                        f"sz_sem{i}": DMA((layers,)), f"rz_sem{i}": DMA((layers, 28))})
    return res


def layers_kernel(w_hbm, feat, row_in, live_in, col_in, bias, out, *refs):
    f32, bf16 = jnp.float32, jnp.bfloat16
    s = dict(zip(scratch(LAYERS), refs))
    pack, inb, outb, meta, biasv, wbuf = (s[n] for n in ("pack", "inb", "outb", "meta", "biasv", "wbuf"))
    metav, colv, metas, cols, cmeta = (s[n] for n in ("metav", "colv", "metas", "cols", "cmeta"))
    nx, ny, im = lax.axis_index("nx"), lax.axis_index("ny"), lax.axis_index("img")
    x, c = nx // 2, nx % 2
    yl, z = ny // NZ, ny % NZ
    me = yl * 2 + c
    plane = x * NZ + z
    flat = nx * NY + ny
    layers = LAYERS

    def dev(xx, cc, yy, zz, ii):
        return (xx * 2 + cc, yy * NZ + zz, ii)

    partner = dev(x, 1 - c, yl, z, im)
    near = dev(x, c, 1 - yl, z, im)
    diag = dev(x, 1 - c, 1 - yl, z, im)
    im_up = (im + yl) % 2
    im_dn = (im + 1 - yl) % 2
    x1, x2, x3 = (x + 1) % NXC, (x + 2) % NXC, (x + 3) % NXC
    xp, xm = dev(x1, c, yl, z, im), dev(x3, c, yl, z, im)

    def along_z(hops):
        return dev(x, c, yl, (z + NZ + hops) % NZ, im)

    def plus(k):
        return k % 2 == 1 or k == 0

    def col_z(k):
        far = 4 - (k + 1) // 2
        return (z + NZ + jnp.where(k % 2 == 1, far, -far)) % NZ

    spread = (4, 12, 3, 13, 5, 11, 2, 14, 6, 10, 1, 15, 7, 9, 8)

    def for_half(fn):
        def rows(t, carry):
            n = (nx + 4 + (t + 1) // 2 * (1 - 2 * (t % 2))) % (2 * NXC)
            for b in spread + (0,):
                fn(n * NY + (ny + b) % NY, (n, (ny + b) % NY, im))
            return carry

        lax.fori_loop(0, 2 * NXC - 1, rows, 0)
        for b in spread:
            fn(nx * NY + (ny + b) % NY, (nx, (ny + b) % NY, im))

    def for_plane(fn):
        def step(j, carry):
            fn(j, dev((x + j // NZ) % NXC, c, yl, (z + j) % NZ, im))
            return carry

        lax.fori_loop(1, NXC * NZ, step, 0)

    def remote(src, dst, ss, rs, d):
        return pltpu.make_async_remote_copy(src_ref=src, dst_ref=dst, send_sem=ss, recv_sem=rs,
                                            device_id=d, device_id_type=MESH)

    barrier = pltpu.get_barrier_semaphore()

    def greet(k, d):
        pl.semaphore_signal(barrier, inc=1, device_id=d, device_id_type=MESH)

    for cc in (0, 1):
        greet(0, dev(x, cc, 1 - yl, z, 1 - im))
    for_half(greet)
    for r in range(4):
        pack[:, r, :] = feat[:, r, 0, :]
    for i in range(layers):
        meta[i, :] = row_in[i, 0, :]
        meta[3 + i, :] = live_in[i, 0, :]
        cmeta[i, :] = col_in[i, 0, :]
        for r in range(4):
            biasv[i, r, 0, :] = bias[i, r * 128:(r + 1) * 128]
    cmeta[3, :] = cmeta[0, :]
    meta[6, :] = meta[0, :]
    meta[7, :] = meta[0, :]
    metav[me] = meta[...]
    colv[plane] = cmeta[...]
    pl.semaphore_wait(barrier, 2 + HALF - 1)

    for_half(lambda k, d: remote(pack.at[k], inb.at[flat], s["in_s"], s["in_r"], d).start())

    def meta_cp(k, d):
        return remote(meta, metav.at[me], s["ms_sem"].at[k], s["mr_sem"].at[k], d)

    group = ((0, partner, yl * 2 + 1 - c), (1, near, (1 - yl) * 2 + c), (2, diag, (1 - yl) * 2 + 1 - c))
    for k, d, _ in group:
        meta_cp(k, d).start()

    def start_weights(l, lo, hi):
        def column_copies(k, both):
            zz = col_z(k)

            def send(x0, n, cc, yy, ii):
                remote(w_hbm.at[l, pl.ds(x0, n), cc, yy, zz], wbuf.at[l, me, k, pl.ds(x0, n)],
                       s["ws_sem"].at[l], s["wr_sem"].at[l, k], dev(x, cc, yy, z, ii)).start()

            for cc in (0, 1):
                if both:
                    send(0, 2, cc, 1 - yl, im_up)
                    send(2, 2, cc, 1 - yl, im_dn)
                else:
                    send(0, 4, cc, 1 - yl, 1 - im)
            send(0, 4, 1 - c, yl, im)
            pltpu.make_async_copy(w_hbm.at[l, :, c, yl, zz], wbuf.at[l, me, k], s["wl_sem"].at[l, k]).start()

        def step(both):
            def run(k, carry):
                column_copies(k, both)
                return carry

            return run

        split = SPLIT if l else NZ
        if lo < split:
            lax.fori_loop(lo, min(hi, split), step(True), 0)
        if hi > split:
            lax.fori_loop(max(lo, split), hi, step(False), 0)

    def wait_weights(l, k):
        pltpu.make_async_copy(w_hbm.at[l, :, c, yl, 0], wbuf.at[l, me, k], s["wl_sem"].at[l, k]).wait()
        three = wbuf.at[l, pl.ds(0, 3), k]
        remote(three, three, s["ws_sem"].at[l], s["wr_sem"].at[l, k], partner).wait_recv()

    start_weights(0, 0, FIRST)
    for_plane(lambda j, d: remote(cmeta, colv.at[plane], s["cs_sem"], s["cr_sem"], d).start())
    inb[flat] = pack[flat]
    lot = remote(pack.at[pl.ds(0, HALF - 1)], inb.at[pl.ds(0, HALF - 1)], s["in_s"], s["in_r"], partner)
    lot.wait_recv()
    for r in range(4):
        rows = inb[:, r, :]
        for i, (_, m) in enumerate(STREAMS):
            s[f"act{i}"][0, me, r] = rows[OFFSET[i]:OFFSET[i] + m]

    tables = (pltpu.make_async_copy(metav, metas, s["loc_sem"].at[0]),
              pltpu.make_async_copy(colv, cols, s["loc_sem"].at[1]))

    def take_tables():
        for k, d, src in group:
            remote(meta, metav.at[src], s["ms_sem"].at[k], s["mr_sem"].at[k], d).wait_recv()
            meta_cp(k, d).wait_send()
        most = colv.at[pl.ds(0, NXC * NZ - 1)]
        most = remote(most, most, s["cs_sem"], s["cr_sem"], partner)
        most.wait_recv()
        most.wait_send()
        for cp in tables:
            cp.start()

    def ag(l, i, src, slot, d):
        ref = s[f"act{i}"].at[l, src]
        return remote(ref, ref, s[f"ag_s{i}"].at[l, slot], s[f"ag_r{i}"].at[l, slot], d)

    def ags(l, i, _):
        ag(l, i, me, 0, near).start()
        ag(l, i, me, 1, partner).start()

    def fwd(l, i, _):
        ag(l, i, (1 - yl) * 2 + c, 0, near).wait_recv()
        ag(l, i, (1 - yl) * 2 + c, 2, partner).start()

    def sent(l, i):
        for slot in range(3):
            ag(l, i, me, slot, partner).wait_send()
        for a in "xz":
            ref = s[f"r{a}{i}"].at[l]
            remote(ref, ref, s[f"s{a}_sem{i}"].at[l], s["in_r"], partner).wait_send()

    def work(l, i, _):
        ag(l, i, yl * 2 + 1 - c, 1, partner).wait_recv()
        ag(l, i, (1 - yl) * 2 + 1 - c, 2, partner).wait_recv()
        if l > 0:
            sent(l - 1, i)
        for src in range(4):
            s[f"work{i}"][src] = s[f"act{i}"][l, src]

    arrived = set()

    def col(l, i, seg):
        kind, _ = STREAMS[i]
        ks = SEGS[min(l, 1)][seg]
        for k in ks:
            if (l, k) not in arrived:
                arrived.add((l, k))
                wait_weights(l, k)
        held, yf = s[f"work{i}"], s[f"yf{i}"]

        def product(k, xx, zz):
            dest = (xx * 2 + c) * NY + yl * NZ + zz
            parts = [None] * 4
            for src in range(4):
                at = (x * 2 + src % 2) * NY + (src // 2) * NZ + z
                row, live, place = metas[src, l, dest], metas[src, 3 + l, dest], cols[xx * NZ + zz, l, at]
                term = jnp.dot(held[src, row], wbuf[l, src, k, xx], preferred_element_type=f32)
                key = jnp.where(live == 1, place, 4)
                for q in range(4):
                    mine = jnp.where(key == q, term, jnp.zeros_like(term))
                    parts[q] = mine if src == 0 else parts[q] + mine
            return parts

        def step(t, carry):
            k, p = t // 2, t % 2
            zz = col_z(k)
            up = jnp.where(jnp.logical_or(k % 2 == 1, k == 0), 1, 0)
            near_x = jnp.where(up == 1, x1, x3)
            far_x = jnp.where(up == 1, x3, x1)
            one = product(k, jnp.where(p == 0, x2, far_x), zz)
            two = product(k, jnp.where(p == 0, near_x, x), zz)
            for q in range(4):
                a, b = one[q], two[q]
                if kind == 0:
                    s[f"yb{i}"][k, p, q] = a.astype(bf16)
                    yf[k, p, q] = b
                else:
                    yf[k, p * (1 + up), q] = a
                    yf[k, 3 * p + (1 - p) * (2 - up), q] = b
            return carry

        lax.fori_loop(2 * ks[0], 2 * ks[-1] + 2, step, 0)

    def xa(l, i, k, n, src, d):
        return remote(src, s[f"rx{i}"].at[l, n, k], s[f"sx_sem{i}"].at[l], s[f"rx_sem{i}"].at[l, n, k], d)

    def s1(l, i, k):
        xa(l, i, k, 0, s[f"yb{i}"].at[k, 0], xp if plus(k) else xm).start()

    def imm(l, i, k):
        xa(l, i, k, 1, s[f"yb{i}"].at[k, 1], xm if plus(k) else xp).start()

    def acc(l, i, k):
        xa(l, i, k, 0, s[f"sx{i}"].at[k], xp).wait_recv()
        s[f"sx{i}"][k] = (s[f"yf{i}"][k, 0] + s[f"rx{i}"][l, 0, k].astype(f32)).astype(bf16)
        xa(l, i, k, 2, s[f"sx{i}"].at[k], xp if plus(k) else xm).start()

    def za(l, i, k):
        hops = JOIN[k][0]
        return remote(s[f"sz{i}"].at[k], s[f"rz{i}"].at[l, k], s[f"sz_sem{i}"].at[l], s[f"rz_sem{i}"].at[l, k],
                      along_z(hops if plus(k) else -hops))

    def total(l, i, k):
        for n in (1, 2):
            xa(l, i, k, n, s[f"sx{i}"].at[k], xp).wait_recv()
        val = (s[f"yf{i}"][k, 1] + s[f"rx{i}"][l, 1, k].astype(f32)) + s[f"rx{i}"][l, 2, k].astype(f32)
        for j in range(7):
            if JOIN[j][1] == k:
                za(l, i, j).wait_recv()
                val = val + s[f"rz{i}"][l, j].astype(f32)
        if k < 7:
            s[f"sz{i}"][k] = val.astype(bf16)
            za(l, i, k).start()
        else:
            s[f"act{i}"][l + 1, me] = jnp.maximum(val + biasv[l], 0.0).astype(bf16)

    def zb(l, i, side, level, role):
        n = bslot(side, level, role)
        return remote(s[f"sz{i}"].at[n], s[f"rz{i}"].at[l, n], s[f"sz_sem{i}"].at[l], s[f"rz_sem{i}"].at[l, n],
                      along_z(-1 if side else 1))

    def b_step(l, i, level, side, role):
        n = bslot(side, level, role)
        val = s[f"yf{i}"][(UP, DOWN)[side][level], role]
        if level > 1 or (level == 1 and role // 2 == side):
            zb(l, i, side, level - 1, role).wait_recv()
            val = val + s[f"rz{i}"][l, bslot(side, level - 1, role)].astype(f32)
        s[f"sz{i}"][n] = val.astype(bf16)
        zb(l, i, side, level, role).start()

    def xb(l, i, n, d):
        return remote(s[f"sx{i}"].at[n], s[f"rx{i}"].at[l, n], s[f"sx_sem{i}"].at[l], s[f"rx_sem{i}"].at[l, n], d)

    def b_sum(l, i, role):
        val = s[f"yf{i}"][7, role]
        for side in (0, 1):
            zb(l, i, side, 3, role).wait_recv()
            val = val + s[f"rz{i}"][l, bslot(side, 3, role)].astype(f32)
        return val

    def b_far(l, i, _):
        val = b_sum(l, i, 0)
        for n, d in ((0, xp), (1, xm)):
            s[f"sx{i}"][n] = val[2 * n:2 * n + 2].astype(bf16)
            xb(l, i, n, d).start()

    def b_imm(l, i, side):
        val = b_sum(l, i, 1 + side)
        n, hi, lo = 3 + 2 * side, 2 - 2 * side, 2 * side
        s[f"sx{i}"][n] = val[hi:hi + 2].astype(bf16)
        xb(l, i, n, xm if side else xp).start()
        s[f"yf{i}"][7, 1 + side, lo:lo + 2] = val[lo:lo + 2]

    def b_acc(l, i, side):
        n, lo = 2 + 2 * side, 2 * side
        xb(l, i, side, xp).wait_recv()
        s[f"sx{i}"][n] = (s[f"yf{i}"][7, 1 + side, lo:lo + 2] + s[f"rx{i}"][l, side].astype(f32)).astype(bf16)
        xb(l, i, n, xm if side else xp).start()

    def b_own(l, i, _):
        s[f"yf{i}"][7, 3] = b_sum(l, i, 3)

    def fin(l, i, _):
        if STREAMS[i][0] == 0:
            total(l, i, 7)
            return
        for n in range(2, 6):
            xb(l, i, n, xp).wait_recv()
        for lo, a, b in ((0, 2, 5), (2, 3, 4)):
            val = s[f"yf{i}"][7, 3, lo:lo + 2] + s[f"rx{i}"][l, a].astype(f32) + s[f"rx{i}"][l, b].astype(f32)
            s[f"act{i}"][l + 1, me, lo:lo + 2] = jnp.maximum(val + biasv[l, lo:lo + 2], 0.0).astype(bf16)

    steps = {AGS: ags, FWD: fwd, WORK: work, COL: col, S1: s1, IM: imm, AC: acc, TO: total, FIN: fin,
             B0: lambda l, i, r: b_step(l, i, 0, r // 2, r), BF: b_far, BI: b_imm, BA: b_acc, BO: b_own}
    for level, name in ((1, B1), (2, B2), (3, B3)):
        steps[name] = lambda l, i, a, level=level: b_step(l, i, level, a // 4, a % 4)
    count = {}
    tables_held = False
    for name, l, i, arg in ORDER:
        if name == COL and not tables_held:
            tables_held = True
            for cp in tables:
                cp.wait()
        steps[name](l, i, arg)
        if name == AGS and l == 0 or name == FWD:
            count[name, l] = count.get((name, l), 0) + 1
            if count[name, l] == len(STREAMS):
                if name == AGS:
                    start_weights(0, FIRST, NZ)
                    take_tables()
                elif l < layers - 1:
                    start_weights(l + 1, 0, NZ)

    for r in range(4):
        for i, (_, m) in enumerate(STREAMS):
            outb[pl.ds(OFFSET[i], m), r, :] = s[f"act{i}"][layers, me, r]
    for_half(lambda k, d: remote(outb.at[k], out.at[flat], s["out_s"], s["out_r"], d).start())
    out[flat] = outb[flat]
    lot.wait_send()
    for i in range(len(STREAMS)):
        sent(layers - 1, i)
    for l in range(layers):
        three = wbuf.at[l, pl.ds(0, 3)]
        remote(three, three, s["ws_sem"].at[l], s["wr_sem"].at[l, 0], partner).wait_send()
    lot = remote(outb.at[pl.ds(0, HALF - 1)], out.at[pl.ds(0, HALF - 1)], s["out_s"], s["out_r"], partner)
    lot.wait_recv()
    lot.wait_send()


def run_layers(w, feat, row, live, col, bias):
    vm = pl.BlockSpec(memory_space=pltpu.VMEM)
    return pl.pallas_call(
        layers_kernel,
        out_shape=jax.ShapeDtypeStruct((HALF, 4, 128), jnp.bfloat16),
        in_specs=[pl.BlockSpec(memory_space=pl.ANY)] + [vm] * 5,
        out_specs=vm,
        scratch_shapes=list(scratch(LAYERS).values()),
        compiler_params=pltpu.CompilerParams(
            collective_id=0, has_side_effects=True, vmem_limit_bytes=60 * 1024 * 1024),
    )(w, feat, row, live, col, bias)


def local(features, link_weight, link_row, link_col, link_live, bias):
    layers = bias.shape[0]
    res = run_layers(link_weight.reshape(layers, NXC, 2, 2, NZ, 128, 128), features.reshape(HALF, 4, 1, 128),
                     link_row, link_live, link_col.transpose(0, 2, 1), bias)
    return res.reshape(features.shape)


def solution(mesh):
    placed = (
        P(("nx", "ny", "img"), None),
        P(None, ("nx", "ny"), None, None, None),
        P(None, ("nx", "ny"), None),
        P(None, None, ("nx", "ny")),
        P(None, ("nx", "ny"), None),
        P(None, ("nx", "ny")),
    )
    return jax.shard_map(
        local, mesh=mesh, in_specs=placed, out_specs=P(("nx", "ny", "img"), None), check_vma=False
    )
```
